8 devices in a mesh: dp: 2 (over y, z), tp: 4 (over x, core).
Axes of the slice: x: 2, y: 2, z: 1, core: 2. Of those that a mesh axis runs over, the one named last changes fastest.
Arguments:
- x: bfloat16 [2048, 6656], P(('dp', 'tp')), parts along dimension 0
- gain: bfloat16 [6656], replicated
- wq: bfloat16 [6656, 6656], P(None, 'tp')
- wk: bfloat16 [6656, 6656], P(None, 'tp')
- wv: bfloat16 [6656, 6656], P(None, 'tp')
- wo: bfloat16 [6656, 6656], P('tp')
Outputs:
- output: bfloat16 [2048, 6656], P(('dp', 'tp')), parts along dimension 0
There are 2 independent parts. The reference program is written for one: setup_inputs(seed, part) draws one part's arguments, and reference() takes and returns one part's arrays. A program takes and returns all parts, laid end to end along the dimension named above; an argument that names none is the same for every part.
All inputs are finite; a program needn't handle non-finite values.
Results may differ from the reference program's by a relative error of at most 0.012.
Values are sent between devices in bfloat16 or wider.
A program may use at most 2 GiB of HBM per device.

```python
import jax
import jax.numpy as jnp
from jax import lax

ROWS = 1024
D = 6656
HEADS = 52
KV_HEADS = 52
HEAD = 128
THETA = 10000


def setup_inputs(seed: int = 0, part: int = 0) -> dict:
    kx, kn, kq, kk, kv, ko = jax.random.split(jax.random.key(seed), 6)

    def weights(key, rows, columns):
        return jax.random.normal(key, (rows, columns), jnp.float32) * rows**-0.5

    drawn = {
        "x": jax.random.normal(jax.random.fold_in(kx, part), (ROWS, D), jnp.float32),
        "gain": 1 + 0.1 * jax.random.normal(kn, (D,), jnp.float32),
        "wq": 2 * weights(kq, D, HEADS * HEAD),
        "wk": 2 * weights(kk, D, KV_HEADS * HEAD),
        "wv": 4 * weights(kv, D, KV_HEADS * HEAD),
        "wo": weights(ko, HEADS * HEAD, D),
    }
    return {k: v.astype(jnp.bfloat16) for k, v in drawn.items()}


def normed(x, gain):
    wide = x.astype(jnp.float32)
    scale = lax.rsqrt(jnp.mean(wide * wide, -1, keepdims=True) + 1e-6)
    return (wide * scale * gain.astype(jnp.float32)).astype(jnp.bfloat16)


def turned(t, place, theta):
    half = t.shape[-1] // 2
    angle = place.astype(jnp.float32)[:, None] * theta ** (-jnp.arange(half, dtype=jnp.float32) / half)
    cos, sin = jnp.cos(angle)[:, None], jnp.sin(angle)[:, None]
    a, b = t[..., :half].astype(jnp.float32), t[..., half:].astype(jnp.float32)
    return jnp.concatenate([a * cos - b * sin, b * cos + a * sin], -1).astype(jnp.bfloat16)


def matmul(a, w):
    return jnp.dot(a, w, preferred_element_type=jnp.float32).astype(jnp.bfloat16)


def einsum(form, a, b):
    return jnp.einsum(form, a.astype(jnp.float32), b.astype(jnp.float32))


def attention(q, k, v):
    scores = einsum("tgsd,ugd->gstu", q, k) * q.shape[-1] ** -0.5
    token = jnp.arange(q.shape[0])
    scores = jnp.where(token[:, None] >= token, scores, -jnp.inf)
    weights = jax.nn.softmax(scores, -1).astype(jnp.bfloat16)
    return einsum("gstu,ugd->tgsd", weights, v).astype(jnp.bfloat16)


def reference(x, gain, wq, wk, wv, wo):
    a, place = normed(x, gain), jnp.arange(ROWS)
    q = turned(matmul(a, wq).reshape(ROWS, HEADS, HEAD), place, THETA).reshape(ROWS, KV_HEADS, -1, HEAD)
    k = turned(matmul(a, wk).reshape(ROWS, KV_HEADS, HEAD), place, THETA)
    v = matmul(a, wv).reshape(ROWS, KV_HEADS, HEAD)
    seen = attention(q, k, v).reshape(ROWS, HEADS * HEAD)
    return (x.astype(jnp.float32) + jnp.dot(seen, wo, preferred_element_type=jnp.float32)).astype(jnp.bfloat16)
```

```python
import functools

import jax
import jax.numpy as jnp
import numpy as np
from jax import lax
from jax.experimental import pallas as pl
from jax.experimental.pallas import tpu as pltpu
from jax.sharding import PartitionSpec as P

HEAD = 128
THETA = 10000
NEG = -1e30
HIDDEN = 2 * NEG
LOG2E = 1.4426950408889634
MESH = pl.DeviceIdType.MESH
BF, F32 = jnp.bfloat16, jnp.float32

D = 6656
ROWS = 256
HEADS = 13
WIDTH = HEADS * HEAD
HALF = D // 2
TILE = 512
QT = 10
OT = D // TILE
SLOTS = 4
LOCAL = 2 * QT * 2
PIECE = QT * 2 + OT
REMOTE = LOCAL + 2 * PIECE
CHUNKS = REMOTE + 2 * OT
SUB = 4
PART = ROWS // SUB
GROUPS = ((0, 1, 2, 3), (4, 5, 6, 7), (8, 9, 10, 11, 12))


def rope_tables():
    half = HEAD // 2
    place = np.arange(4 * ROWS, dtype=np.float32)[:, None]
    angle = place * np.power(np.float32(THETA), -np.arange(half, dtype=np.float32) / np.float32(half))
    cos, sin = np.cos(angle), np.sin(angle)
    cos = np.concatenate([np.concatenate([cos, cos], 1), np.ones((ROWS, HEAD))], 0)
    sin = np.concatenate([np.concatenate([-sin, sin], 1), np.zeros((ROWS, HEAD))], 0)
    return cos.astype(np.float32), sin.astype(np.float32)


def cols(n):
    return pl.ds(pl.multiple_of(n * TILE, TILE), TILE)


def rows_of(block):
    return pl.ds(pl.multiple_of(block * ROWS, ROWS), ROWS)


def kernel(x, gain, wq, wk, wv, wo, cos_h, sin_h, y,
           a, qkv, seen, w, r_in, l_in, g_out, d_out, d_in, acc, raw, cos, sin, top_s, mix_s, gap_s,
           w_sem, x_sem, t_sem, swap_s, swap_r, link_s, link_r, pass_s, pass_r, d_s, d_r, rs_s, rs_r, l_s, l_r, y_sem):
    me = lax.axis_index("tp")
    c = lax.rem(me, 2)
    far = 1 - lax.div(me, 2)
    peer = me + 1 - 2 * c
    across = far * 2 + c
    diagonal = far * 2 + 1 - c

    def remote(src, dst, s, r, to):
        return pltpu.make_async_remote_copy(src_ref=src, dst_ref=dst, send_sem=s, recv_sem=r, device_id={"tp": to}, device_id_type=MESH)

    def issue(g):
        slot = lax.rem(g, SLOTS)
        past = jnp.maximum(g - LOCAL, 0)
        in_piece = lax.rem(past, PIECE)
        remote_part = (g >= LOCAL) & (g < REMOTE)
        out = (g >= REMOTE) | (remote_part & (in_piece >= 2 * QT))
        chunk = jnp.where(g < LOCAL, g, in_piece)
        t = lax.rem(lax.div(chunk, 2), QT)
        n = jnp.where(g >= REMOTE, lax.rem(jnp.maximum(g - REMOTE, 0), OT), jnp.maximum(in_piece - 2 * QT, 0))
        deep = pl.ds(pl.multiple_of(lax.rem(chunk, 2) * HALF, HALF), HALF)
        project = (g < REMOTE) & jnp.logical_not(out)
        for i, ref in enumerate((wq, wk, wv)):

            @pl.when(project & (t >= 3 * i) & (t < 3 * i + 3))
            def _(i=i, ref=ref):
                pltpu.make_async_copy(ref.at[deep, cols(lax.rem(t, 3))], w.at[slot], w_sem.at[slot]).start()

        @pl.when(project & (t == QT - 1))
        def _():
            for i, ref in enumerate((wq, wk, wv, wv)):
                pltpu.make_async_copy(
                    ref.at[deep, pl.ds(3 * TILE, HEAD)], w.at[slot, :, pl.ds(i * HEAD, HEAD)], w_sem.at[slot]
                ).start()

        @pl.when(out & (g < CHUNKS))
        def _():
            pltpu.make_async_copy(wo.at[:, cols(n)], w.at[slot, pl.ds(0, WIDTH)], w_sem.at[slot]).start()

    def projection_chunk(g):
        issue(g + SLOTS - 1)
        slot = lax.rem(g, SLOTS)
        pltpu.make_async_copy(wq.at[pl.ds(0, HALF), pl.ds(0, TILE)], w.at[slot], w_sem.at[slot]).wait()
        return slot

    def output_chunk(g):
        issue(g + SLOTS - 1)
        slot = lax.rem(g, SLOTS)
        pltpu.make_async_copy(wo.at[:, pl.ds(0, TILE)], w.at[slot, pl.ds(0, WIDTH)], w_sem.at[slot]).wait()
        return slot

    def part(block, s):
        return a.at[pl.ds(pl.multiple_of(block * ROWS + s * PART, PART), PART)]

    def swap(s):
        return remote(part(me, s), part(me, s), swap_s.at[s], swap_r.at[s], peer)

    def link(s):
        return remote(part(me, s), part(me, s), link_s.at[s], link_r.at[s], across)

    def passed(s):
        return remote(part(across, s), part(across, s), pass_s.at[s], pass_r.at[s], peer)

    def pass_on(s):
        link(s).wait_recv()
        passed(s).start()

    loads = [pltpu.make_async_copy(x.at[pl.ds(s * PART, PART)], g_out.at[pl.ds(s * PART, PART)], x_sem.at[s]) for s in range(SUB)]
    tables = [pltpu.make_async_copy(cos_h, cos, t_sem.at[0]), pltpu.make_async_copy(sin_h, sin, t_sem.at[1])]
    for copy in loads:
        copy.start()
    for copy in tables:
        copy.start()
    for g in range(SLOTS - 1):
        issue(jnp.int32(g))
    barrier = pltpu.get_barrier_semaphore()
    for to in (peer, across, diagonal):
        pl.semaphore_signal(barrier, inc=1, device_id={"tp": to}, device_id_type=MESH)
    pl.semaphore_wait(barrier, 3)

    def send(s):
        swap(s).start()

        @pl.when(c == 0)
        def _():
            link(s).start()

    for s in range(SUB):
        loads[s].wait()

        def norm(i, _, s=s):
            at = s * PART + i * 16
            wide = g_out[pl.ds(at, 16), :].astype(F32)
            scale = lax.rsqrt(jnp.mean(wide * wide, -1, keepdims=True) + 1e-6)
            a[pl.ds(pl.multiple_of(me * ROWS + at, 16), 16), :] = (wide * scale * gain[...].astype(F32)).astype(BF)

        lax.fori_loop(0, PART // 16, norm, None)
        if s:
            send(s - 1)
    gap_s[...] = lax.broadcasted_iota(jnp.int32, (ROWS, ROWS), 1) - lax.broadcasted_iota(jnp.int32, (ROWS, ROWS), 0)
    for copy in tables:
        copy.wait()
    send(SUB - 1)

    def turn(t, block, at):
        for i in range(4):
            slot = jnp.where(t < QT - 1, lax.div(t, 3) * HEADS + lax.rem(t, 3) * 4 + i, min(i * HEADS + HEADS - 1, 3 * HEADS))
            plain = ((t >= 6) & (t < QT - 1)) | ((t == QT - 1) & (i >= 2))
            angles = pl.ds(pl.multiple_of(jnp.where(plain, 4, block) * ROWS, ROWS), ROWS)
            v = raw[at, :, pl.ds(i * HEAD, HEAD)].astype(F32)
            v = v * cos[angles, :] + pltpu.roll(v, HEAD // 2, 1) * sin[angles, :]
            qkv[slot, rows_of(block), :] = v.astype(BF)

    def project(g, t, block, before):
        slot = projection_chunk(g)
        acc[0] = jnp.dot(a[rows_of(block), pl.ds(0, HALF)], w[slot], preferred_element_type=F32)
        slot = projection_chunk(g + 1)
        here = lax.rem(t, 2)
        raw[here] = (acc[0] + jnp.dot(a[rows_of(block), pl.ds(HALF, HALF)], w[slot], preferred_element_type=F32)).astype(BF)
        if before is not None:
            turn(*before)

    def local(i, _):
        t, block = lax.rem(i, QT), jnp.where(i < QT, me, peer)
        late = jnp.maximum(i - 1, 0)

        @pl.when(i == QT)
        def _():
            for s in range(SUB):
                swap(s).wait_recv()

        @pl.when((c == 1) & (i == 15))
        def _():
            for s in range(SUB):
                link(s).start()

        for s in range(SUB):

            @pl.when((c == 0) & (i == 4 * s + 6))
            def _(s=s):
                pass_on(s)

        project(2 * i, t, block, (lax.rem(late, QT), jnp.where(late < QT, me, peer), lax.rem(late, 2)))

    raw[...] = jnp.zeros_like(raw)
    lax.fori_loop(0, 2 * QT, local, None)
    turn(jnp.int32(QT - 1), peer, (QT - 1) % 2)

    def attend(block):
        e = HEAD**-0.5 * LOG2E
        top_s[...] = jnp.full(top_s.shape, NEG, F32)
        mix_s[...] = jnp.zeros(mix_s.shape, F32)
        ones = jnp.ones((8, ROWS), BF)

        def keys(j, _):
            ok = gap_s[...] >= (j - block) * ROWS
            for heads in GROUPS:
                scores = [
                    lax.dot_general(qkv[HEADS + h, rows_of(j), :], qkv[h, rows_of(block), :], (((1,), (1,)), ((), ())), preferred_element_type=F32)
                    for h in heads
                ]
                weights, keeps = [], []
                for h, s in zip(heads, scores):
                    s = jnp.where(ok, s, HIDDEN)
                    old = top_s[h : h + 1, :]
                    top = jnp.maximum(old, s.max(axis=0, keepdims=True))
                    top_s[h : h + 1, :] = top
                    weights.append(jnp.exp2((s - top) * e).astype(BF))
                    keeps.append(jnp.exp2((old - top) * e))
                for h, p, keep in zip(heads, weights, keeps):
                    values = jnp.concatenate([qkv[2 * HEADS + h, rows_of(j), :].T, ones], axis=0)
                    mix_s[h] = mix_s[h] * keep + jnp.dot(values, p, preferred_element_type=F32)

        lax.fori_loop(0, block + 1, keys, None)
        for h in range(HEADS):
            done = mix_s[h, :HEAD, :] * (1 / mix_s[h, HEAD : HEAD + 1, :])
            seen[rows_of(block), pl.ds(h * HEAD, HEAD)] = done.T.astype(BF)

    def output(g, block):
        slot = output_chunk(g)
        return jnp.dot(seen[rows_of(block), :], w[slot, pl.ds(0, WIDTH), :], preferred_element_type=F32)

    mine = pl.ds(pl.multiple_of(c * 128, 128), 128)
    others = pl.ds(pl.multiple_of((1 - c) * 128, 128), 128)

    def exchange(q):
        slot = lax.rem(q, 4)
        return remote(d_out.at[slot], d_in.at[slot], d_s.at[slot], d_r.at[slot], peer)

    def back(p, n):
        src = g_out.at[pl.ds(pl.multiple_of(p * 128, 128), 128), cols(n)]
        return remote(src, r_in.at[mine, cols(n)], rs_s.at[p, n], rs_r.at[c, n], far * 2 + p)

    def piece(p, _):
        block = far * 2 + p
        base = LOCAL + p * PIECE

        @pl.when(c != p)
        def _():
            for s in range(SUB):
                passed(s).wait_recv()

        def tiles(t, _):
            for s, i in ((0, 2), (1, 7)):

                @pl.when((c == 1) & (p == 0) & (t == i))
                def _(s=s):
                    pass_on(s)

            late = jnp.maximum(t - 1, 0)
            project(base + 2 * t, t, block, (late, block, lax.rem(late, 2)))

        lax.fori_loop(0, QT, tiles, None)
        turn(jnp.int32(QT - 1), block, (QT - 1) % 2)
        attend(block)

        @pl.when((c == 1) & (p == 0))
        def _():
            pass_on(2)

        def add(n):
            q = p * OT + n
            exchange(q).wait_recv()
            total = acc[lax.rem(n, 2), mine, :] + d_in[lax.rem(q, 4)].astype(F32)
            g_out[pl.ds(pl.multiple_of(p * 128, 128), 128), cols(n)] = total.astype(BF)

        def tiles_out(n, _):
            q = p * OT + n

            @pl.when((c == 1) & (p == 0) & (n == 6))
            def _():
                pass_on(3)

            acc[lax.rem(n, 2)] = output(base + 2 * QT + n, block)

            @pl.when(q >= 4)
            def _():
                exchange(q - 4).wait_send()

            d_out[lax.rem(q, 4)] = acc[lax.rem(n, 2), others, :].astype(BF)

            @pl.when(n >= 1)
            def _():
                add(n - 1)

            exchange(q).start()

            @pl.when(n >= 2)
            def _():
                back(p, n - 2).start()

        lax.fori_loop(0, OT, tiles_out, None)
        back(p, OT - 2).start()
        add(OT - 1)
        back(p, OT - 1).start()

    lax.fori_loop(0, 2, piece, None)
    for q in range(2 * OT - 4, 2 * OT):
        exchange(jnp.int32(q)).wait_send()

    for s in range(SUB):
        swap(s).wait_send()
        link(s).wait_send()
        passed(s).wait_send()
    again = pltpu.make_async_copy(x, a.at[pl.ds(3 * ROWS, ROWS)], x_sem.at[0])
    again.start()

    def own_chip(i, _):
        attend((1 - far) * 2 + i)

    lax.fori_loop(0, 2, own_chip, None)

    def give(n):
        return remote(a.at[pl.ds(0, ROWS), cols(n)], l_in.at[:, cols(n)], l_s.at[n], l_r.at[n], peer)

    def tiles_peer(n, _):
        a[pl.ds(0, ROWS), cols(n)] = output(REMOTE + n, peer).astype(BF)

        @pl.when(n >= 1)
        def _():
            give(n - 1).start()

    lax.fori_loop(0, OT, tiles_peer, None)

    def keep(n):
        return pltpu.make_async_copy(a.at[pl.ds(2 * ROWS, ROWS), cols(n)], y.at[:, cols(n)], y_sem.at[n])

    again.wait()
    give(OT - 1).start()

    def tiles_mine(n, _):
        acc[0] = output(REMOTE + OT + n, me)
        give(n).wait_recv()
        for half in range(2):
            remote(g_out.at[pl.ds(0, 128), cols(n)], r_in.at[pl.ds(half * 128, 128), cols(n)], rs_s.at[0, n], rs_r.at[half, n], across).wait_recv()
        total = acc[0] + l_in[:, cols(n)].astype(F32) + r_in[:, cols(n)].astype(F32)
        a[pl.ds(2 * ROWS, ROWS), cols(n)] = (a[pl.ds(3 * ROWS, ROWS), cols(n)].astype(F32) + total).astype(BF)

        @pl.when(n >= 1)
        def _():
            keep(n - 1).start()

    lax.fori_loop(0, OT, tiles_mine, None)

    def ends(n, _):
        give(n).wait_send()
        for p in range(2):
            back(p, n).wait_send()

    lax.fori_loop(0, OT, ends, None)
    keep(OT - 1).start()

    def kept(n, _):
        keep(n).wait()

    lax.fori_loop(0, OT, kept, None)


def solution(mesh):
    tables = rope_tables()

    def step(x, gain, wq, wk, wv, wo):
        anywhere, vmem, dma = pl.BlockSpec(memory_space=pl.ANY), pltpu.VMEM, pltpu.SemaphoreType.DMA
        return pl.pallas_call(
            kernel,
            out_shape=jax.ShapeDtypeStruct((ROWS, D), BF),
            in_specs=[anywhere, pl.BlockSpec(memory_space=pltpu.VMEM)] + [anywhere] * 6,
            out_specs=anywhere,
            scratch_shapes=[
                vmem((4 * ROWS, D), BF),
                vmem((3 * HEADS + 1, 4 * ROWS, HEAD), BF),
                vmem((4 * ROWS, WIDTH), BF),
                vmem((SLOTS, HALF, TILE), BF),
                vmem((ROWS, D), BF),
                vmem((ROWS, D), BF),
                vmem((ROWS, D), BF),
                vmem((4, 128, TILE), BF),
                vmem((4, 128, TILE), BF),
                vmem((2, ROWS, TILE), F32),
                vmem((2, ROWS, TILE), BF),
                vmem((5 * ROWS, HEAD), F32),
                vmem((5 * ROWS, HEAD), F32),
                vmem((16, ROWS), F32),
                vmem((HEADS, HEAD + 8, ROWS), F32),
                vmem((ROWS, ROWS), jnp.int32),
                dma((SLOTS,)),
                dma((SUB,)),
                dma((2,)),
                dma((SUB,)),
                dma((SUB,)),
                dma((SUB,)),
                dma((SUB,)),
                dma((SUB,)),
                dma((SUB,)),
                dma((4,)),
                dma((4,)),
                dma((2, OT)),
                dma((2, OT)),
                dma((OT,)),
                dma((OT,)),
                dma((OT,)),
            ],
            compiler_params=pltpu.CompilerParams(collective_id=0, has_side_effects=True, vmem_limit_bytes=67_043_328),
            name="layer",
        )(x, gain.reshape(1, D), wq, wk, wv, wo, *(jnp.asarray(t) for t in tables))

    tokens, columns = P(("dp", "tp"), None), P(None, "tp")
    return jax.shard_map(
        step,
        mesh=mesh,
        in_specs=(tokens, P(None), columns, columns, columns, P("tp", None)),
        out_specs=tokens,
        check_vma=False,
    )
```

```python
import functools

import jax
import jax.numpy as jnp
import numpy as np
from jax import lax
from jax.experimental import pallas as pl
from jax.experimental.pallas import tpu as pltpu
from jax.sharding import PartitionSpec as P

HEAD = 128
THETA = 10000
NEG = -1e30
HIDDEN = 2 * NEG
LOG2E = 1.4426950408889634
MESH = pl.DeviceIdType.MESH
BF, F32 = jnp.bfloat16, jnp.float32

D = 6656
ROWS = 256
HEADS = 13
WIDTH = HEADS * HEAD
TILE = 512
QT = 10
OT = D // TILE
PAIRS = OT // 2
OU = 4
SLOTS = 3
LOCAL = 2 * QT
PIECE = QT + OU
REMOTE = LOCAL + 2 * PIECE
UNITS = REMOTE + 2 * OU
RING = 3
SUB = 4
PART = ROWS // SUB
GROUPS = ((0, 1, 2, 3), (4, 5, 6, 7), (8, 9, 10, 11, 12))


def rope_tables():
    half = HEAD // 2
    place = np.arange(4 * ROWS, dtype=np.float32)[:, None]
    angle = place * np.power(np.float32(THETA), -np.arange(half, dtype=np.float32) / np.float32(half))
    cos, sin = np.cos(angle), np.sin(angle)
    cos = np.concatenate([np.concatenate([cos, cos], 1), np.ones((ROWS, HEAD))], 0)
    sin = np.concatenate([np.concatenate([-sin, sin], 1), np.zeros((ROWS, HEAD))], 0)
    return cos.astype(np.float32), sin.astype(np.float32)


def cols(n):
    return pl.ds(pl.multiple_of(n * TILE, TILE), TILE)


def rows_of(block):
    return pl.ds(pl.multiple_of(block * ROWS, ROWS), ROWS)


def pair(n):
    return pl.ds(pl.multiple_of(n * 2 * TILE, 2 * TILE), 2 * TILE)


def quarter(j):
    return pl.ds(pl.multiple_of(j * WIDTH, WIDTH), WIDTH)


def kernel(x, gain, wq, wk, wv, wo, cos_h, sin_h, y,
           a, qkv, seen, w, r_in, d_out, d_in, acc, raw, cos, sin, top_s, mix_s, gap_s,
           w_sem, x_sem, t_sem, swap_s, swap_r, link_s, link_r, pass_s, pass_r, d_s, d_r, rs_s, rs_r, l_s, l_r, y_sem):
    me = lax.axis_index("tp")
    c = lax.rem(me, 2)
    far = 1 - lax.div(me, 2)
    peer = me + 1 - 2 * c
    across = far * 2 + c
    diagonal = far * 2 + 1 - c

    def remote(src, dst, s, r, to):
        return pltpu.make_async_remote_copy(src_ref=src, dst_ref=dst, send_sem=s, recv_sem=r, device_id={"tp": to}, device_id_type=MESH)

    def issue(g):
        slot = lax.rem(g, SLOTS)
        in_piece = lax.rem(jnp.maximum(g - LOCAL, 0), PIECE)
        out = (g >= REMOTE) | ((g >= LOCAL) & (in_piece >= QT))
        t = jnp.where(g < LOCAL, lax.rem(g, QT), in_piece)
        u = jnp.where(g >= REMOTE, lax.rem(jnp.maximum(g - REMOTE, 0), OU), jnp.maximum(in_piece - QT, 0))
        project = jnp.logical_not(out)
        for i, ref in enumerate((wq, wk, wv)):

            @pl.when(project & (t >= 3 * i) & (t < 3 * i + 3))
            def _(i=i, ref=ref):
                for j in range(4):
                    pltpu.make_async_copy(ref.at[quarter(j), cols(lax.rem(t, 3))], w.at[slot, quarter(j)], w_sem.at[slot, j]).start()

        @pl.when(project & (t == QT - 1))
        def _():
            for j, ref in enumerate((wq, wk, wv, wv)):
                pltpu.make_async_copy(ref.at[:, pl.ds(3 * TILE, HEAD)], w.at[slot, :, pl.ds(j * HEAD, HEAD)], w_sem.at[slot, j]).start()

        for j in range(4):

            @pl.when(out & (g < UNITS) & (u * 4 + j < OT))
            def _(j=j):
                pltpu.make_async_copy(wo.at[:, cols(u * 4 + j)], w.at[slot, quarter(j)], w_sem.at[slot, j]).start()

    def fetched(slot, j):
        pltpu.make_async_copy(wo.at[:, pl.ds(0, TILE)], w.at[slot, quarter(j)], w_sem.at[slot, j]).wait()

    def part(block, s):
        return a.at[pl.ds(pl.multiple_of(block * ROWS + s * PART, PART), PART)]

    def swap(s):
        return remote(part(me, s), part(me, s), swap_s.at[s], swap_r.at[s], peer)

    def link(s):
        return remote(part(me, s), part(me, s), link_s.at[s], link_r.at[s], across)

    def passed(s):
        return remote(part(across, s), part(across, s), pass_s.at[s], pass_r.at[s], peer)

    def pass_on(s):
        link(s).wait_recv()
        passed(s).start()

    loads = [pltpu.make_async_copy(x.at[pl.ds(s * PART, PART)], r_in.at[pl.ds(s * PART, PART)], x_sem.at[s]) for s in range(SUB)]
    tables = [pltpu.make_async_copy(cos_h, cos, t_sem.at[0]), pltpu.make_async_copy(sin_h, sin, t_sem.at[1])]
    for copy in loads:
        copy.start()
    for copy in tables:
        copy.start()
    for g in range(SLOTS - 1):
        issue(jnp.int32(g))
    barrier = pltpu.get_barrier_semaphore()
    for to in (peer, across, diagonal):
        pl.semaphore_signal(barrier, inc=1, device_id={"tp": to}, device_id_type=MESH)
    pl.semaphore_wait(barrier, 3)

    def send(s):
        swap(s).start()

        @pl.when(c == 0)
        def _():
            link(s).start()

    for s in range(SUB):
        loads[s].wait()

        def norm(i, _, s=s):
            at = s * PART + i * 16
            wide = r_in[pl.ds(at, 16), :].astype(F32)
            scale = lax.rsqrt(jnp.mean(wide * wide, -1, keepdims=True) + 1e-6)
            a[pl.ds(pl.multiple_of(me * ROWS + at, 16), 16), :] = (wide * scale * gain[...].reshape(1, D).astype(F32)).astype(BF)

        lax.fori_loop(0, PART // 16, norm, None)
        if s:
            send(s - 1)
    gap_s[...] = lax.broadcasted_iota(jnp.int32, (ROWS, ROWS), 1) - lax.broadcasted_iota(jnp.int32, (ROWS, ROWS), 0)
    for copy in tables:
        copy.wait()
    send(SUB - 1)

    def turn(t, block, at):
        for i in range(4):
            slot = jnp.where(t < QT - 1, lax.div(t, 3) * HEADS + lax.rem(t, 3) * 4 + i, min(i * HEADS + HEADS - 1, 3 * HEADS))
            plain = ((t >= 6) & (t < QT - 1)) | ((t == QT - 1) & (i >= 2))
            angles = pl.ds(pl.multiple_of(jnp.where(plain, 4, block) * ROWS, ROWS), ROWS)
            v = raw[at, :, pl.ds(i * HEAD, HEAD)].astype(F32)
            v = v * cos[angles, :] + pltpu.roll(v, HEAD // 2, 1) * sin[angles, :]
            qkv[slot, rows_of(block), :] = v.astype(BF)

    def project(g, t, block, before):
        issue(g + SLOTS - 1)
        slot = lax.rem(g, SLOTS)
        for j in range(4):
            fetched(slot, j)
        raw[lax.rem(t, 2)] = jnp.dot(a[rows_of(block), :], w[slot], preferred_element_type=F32).astype(BF)
        turn(*before)

    def local(i, _):
        t, block = lax.rem(i, QT), jnp.where(i < QT, me, peer)
        late = jnp.maximum(i - 1, 0)

        @pl.when(i == QT)
        def _():
            for s in range(SUB):
                swap(s).wait_recv()

        @pl.when((c == 1) & (i == 15))
        def _():
            for s in range(SUB):
                link(s).start()

        for s in range(SUB):

            @pl.when((c == 0) & (i == 4 * s + 6))
            def _(s=s):
                pass_on(s)

        project(i, t, block, (lax.rem(late, QT), jnp.where(late < QT, me, peer), lax.rem(late, 2)))

    raw[...] = jnp.zeros_like(raw)
    lax.fori_loop(0, 2 * QT, local, None)
    turn(jnp.int32(QT - 1), peer, (QT - 1) % 2)

    def attend(block):
        e = HEAD**-0.5 * LOG2E
        top_s[...] = jnp.full(top_s.shape, NEG, F32)
        mix_s[...] = jnp.zeros(mix_s.shape, F32)
        ones = jnp.ones((8, ROWS), BF)

        def keys(j, _):
            ok = gap_s[...] >= (j - block) * ROWS
            for heads in GROUPS:
                scores = [
                    lax.dot_general(qkv[HEADS + h, rows_of(j), :], qkv[h, rows_of(block), :], (((1,), (1,)), ((), ())), preferred_element_type=F32)
                    for h in heads
                ]
                weights, keeps = [], []
                for h, s in zip(heads, scores):
                    s = jnp.where(ok, s, HIDDEN)
                    old = top_s[h : h + 1, :]
                    top = jnp.maximum(old, s.max(axis=0, keepdims=True))
                    top_s[h : h + 1, :] = top
                    weights.append(jnp.exp2((s - top) * e).astype(BF))
                    keeps.append(jnp.exp2((old - top) * e))
                for h, p, keep in zip(heads, weights, keeps):
                    values = jnp.concatenate([qkv[2 * HEADS + h, rows_of(j), :].T, ones], axis=0)
                    mix_s[h] = mix_s[h] * keep + jnp.dot(values, p, preferred_element_type=F32)

        lax.fori_loop(0, block + 1, keys, None)
        for h in range(HEADS):
            done = mix_s[h, :HEAD, :] * (1 / mix_s[h, HEAD : HEAD + 1, :])
            seen[rows_of(block), pl.ds(h * HEAD, HEAD)] = done.T.astype(BF)

    def output(base, block, k, tiles, put):
        slot = lax.rem(base + lax.div(k, 2), SLOTS)
        first = lax.rem(k, 2) * 2

        @pl.when(first == 0)
        def _():
            issue(base + lax.div(k, 2) + SLOTS - 1)

        for j in range(tiles):
            fetched(slot, first + j)
        for j in range(tiles):
            put(j, jnp.dot(seen[rows_of(block), :], w[slot, quarter(first + j), :], preferred_element_type=F32))

    def some(k, tiles):
        return pair(k) if tiles == 2 else pl.ds(PAIRS * 2 * TILE, TILE)

    mine = pl.ds(pl.multiple_of(c * 128, 128), 128)
    others = pl.ds(pl.multiple_of((1 - c) * 128, 128), 128)

    def exchange(q, tiles):
        slot, width = lax.rem(q, RING), pl.ds(0, tiles * TILE)
        return remote(d_out.at[slot, :, width], d_in.at[slot, :, width], d_s.at[slot], d_r.at[slot], peer)

    def sums(p):
        return pl.ds(pl.multiple_of(peer * ROWS + p * 128, 128), 128)

    def back(p, k, tiles):
        return remote(a.at[sums(p), some(k, tiles)], r_in.at[mine, some(k, tiles)], rs_s.at[p, k], rs_r.at[c, k], far * 2 + p)

    def piece(p, _):
        block = far * 2 + p
        base = LOCAL + p * PIECE

        @pl.when(c != p)
        def _():
            for s in range(SUB):
                passed(s).wait_recv()

        def tiles(t, _):
            for s, i in ((0, 2), (1, 7)):

                @pl.when((c == 1) & (p == 0) & (t == i))
                def _(s=s):
                    pass_on(s)

            late = jnp.maximum(t - 1, 0)
            project(base + t, t, block, (late, block, lax.rem(late, 2)))

        lax.fori_loop(0, QT, tiles, None)
        turn(jnp.int32(QT - 1), block, (QT - 1) % 2)
        attend(block)

        @pl.when((c == 1) & (p == 0))
        def _():
            pass_on(2)

        def add(k, tiles):
            q, width = p * (PAIRS + 1) + k, pl.ds(0, tiles * TILE)
            exchange(q, tiles).wait_recv()
            total = acc[lax.rem(k, 2), mine, width] + d_in[lax.rem(q, RING), :, width].astype(F32)
            a[sums(p), some(k, tiles)] = total.astype(BF)

        def tiles_out(k, tiles):
            q, at = p * (PAIRS + 1) + k, lax.rem(k, 2)

            def put(j, value):
                acc[at, :, pl.ds(j * TILE, TILE)] = value

            output(base + QT, block, k, tiles, put)

            @pl.when(k >= 1)
            def _():
                add(k - 1, 2)

            @pl.when((q >= RING) & (lax.rem(q - RING, PAIRS + 1) < PAIRS))
            def _():
                exchange(q - RING, 2).wait_send()

            @pl.when((q >= RING) & (lax.rem(q - RING + PAIRS + 1, PAIRS + 1) == PAIRS))
            def _():
                exchange(q - RING, 1).wait_send()

            d_out[lax.rem(q, RING), :, pl.ds(0, tiles * TILE)] = acc[at, others, pl.ds(0, tiles * TILE)].astype(BF)

            @pl.when(k >= 1)
            def _():
                back(p, k - 1, 2).start()

            exchange(q, tiles).start()

        def pairs_out(k, _):
            @pl.when((c == 1) & (p == 0) & (k == 3))
            def _():
                pass_on(3)

            tiles_out(k, 2)

        @pl.when(p == 1)
        def _():
            for s in range(SUB):
                swap(s).wait_send()
                link(s).wait_send()

        lax.fori_loop(0, PAIRS, pairs_out, None)
        tiles_out(jnp.int32(PAIRS), 1)
        add(jnp.int32(PAIRS), 1)
        back(p, PAIRS, 1).start()

    lax.fori_loop(0, 2, piece, None)
    for q in range(2 * (PAIRS + 1) - RING, 2 * (PAIRS + 1)):
        exchange(jnp.int32(q), 1 if q % (PAIRS + 1) == PAIRS else 2).wait_send()
    for s in range(SUB):
        passed(s).wait_send()
    again = pltpu.make_async_copy(x, a.at[rows_of(diagonal)], x_sem.at[0])
    again.start()

    def own_chip(i, _):
        attend((1 - far) * 2 + i)

    lax.fori_loop(0, 2, own_chip, None)

    def give(k, tiles):
        return remote(a.at[rows_of(across), some(k, tiles)], a.at[rows_of(peer), some(k, tiles)], l_s.at[k], l_r.at[k], peer)

    def tiles_peer(k, tiles):
        def put(j, value):
            a[rows_of(across), pl.ds(pl.multiple_of(k * 2 * TILE + j * TILE, TILE), TILE)] = value.astype(BF)

        output(REMOTE, peer, k, tiles, put)

        @pl.when(k >= 1)
        def _():
            give(k - 1, 2).start()

    lax.fori_loop(0, PAIRS, lambda k, _: tiles_peer(k, 2), None)
    tiles_peer(jnp.int32(PAIRS), 1)

    def keep(k, tiles):
        return pltpu.make_async_copy(a.at[rows_of(diagonal), some(k, tiles)], y.at[:, some(k, tiles)], y_sem.at[k])

    again.wait()
    give(PAIRS, 1).start()

    def tiles_mine(k, tiles):
        def put(j, value):
            acc[0, :, pl.ds(j * TILE, TILE)] = value

        output(REMOTE + OU, me, k, tiles, put)
        here, width = some(k, tiles), pl.ds(0, tiles * TILE)
        remote(a.at[rows_of(across), here], a.at[rows_of(me), here], l_s.at[k], l_r.at[k], peer).wait_recv()
        for half in range(2):
            remote(a.at[sums(0), here], r_in.at[pl.ds(half * 128, 128), here], rs_s.at[0, k], rs_r.at[half, k], across).wait_recv()
        total = acc[0, :, width] + a[rows_of(me), here].astype(F32) + r_in[:, here].astype(F32)
        a[rows_of(diagonal), here] = (a[rows_of(diagonal), here].astype(F32) + total).astype(BF)

        @pl.when(k >= 1)
        def _():
            keep(k - 1, 2).start()

    lax.fori_loop(0, PAIRS, lambda k, _: tiles_mine(k, 2), None)
    tiles_mine(jnp.int32(PAIRS), 1)
    for k in range(PAIRS + 1):
        tiles = 2 if k < PAIRS else 1
        give(k, tiles).wait_send()
        for p in range(2):
            back(p, k, tiles).wait_send()
    keep(PAIRS, 1).start()
    for k in range(PAIRS + 1):
        keep(k, 2 if k < PAIRS else 1).wait()


def solution(mesh):
    tables = rope_tables()

    def step(x, gain, wq, wk, wv, wo):
        anywhere, vmem, dma = pl.BlockSpec(memory_space=pl.ANY), pltpu.VMEM, pltpu.SemaphoreType.DMA
        return pl.pallas_call(
            kernel,
            out_shape=jax.ShapeDtypeStruct((ROWS, D), BF),
            in_specs=[anywhere, pl.BlockSpec(memory_space=pltpu.VMEM)] + [anywhere] * 6,
            out_specs=anywhere,
            scratch_shapes=[
                vmem((4 * ROWS, D), BF),
                vmem((3 * HEADS + 1, 4 * ROWS, HEAD), BF),
                vmem((4 * ROWS, WIDTH), BF),
                vmem((SLOTS, D, TILE), BF),
                vmem((ROWS, D), BF),
                vmem((RING, 128, 2 * TILE), BF),
                vmem((RING, 128, 2 * TILE), BF),
                vmem((2, ROWS, 2 * TILE), F32),
                vmem((2, ROWS, TILE), BF),
                vmem((5 * ROWS, HEAD), F32),
                vmem((5 * ROWS, HEAD), F32),
                vmem((16, ROWS), F32),
                vmem((HEADS, HEAD + 8, ROWS), F32),
                vmem((ROWS, ROWS), jnp.int32),
                dma((SLOTS, 4)),
                dma((SUB,)),
                dma((2,)),
                dma((SUB,)),
                dma((SUB,)),
                dma((SUB,)),
                dma((SUB,)),
                dma((SUB,)),
                dma((SUB,)),
                dma((RING,)),
                dma((RING,)),
                dma((2, PAIRS + 1)),
                dma((2, PAIRS + 1)),
                dma((PAIRS + 1,)),
                dma((PAIRS + 1,)),
                dma((PAIRS + 1,)),
            ],
            compiler_params=pltpu.CompilerParams(collective_id=0, has_side_effects=True, vmem_limit_bytes=67_043_328),
            name="layer",
        )(x, gain, wq, wk, wv, wo, *(jnp.asarray(t) for t in tables))

    tokens, columns = P(("dp", "tp"), None), P(None, "tp")
    return jax.shard_map(
        step,
        mesh=mesh,
        in_specs=(tokens, P(None), columns, columns, columns, P("tp", None)),
        out_specs=tokens,
        check_vma=False,
    )
```

```python
import functools

import jax
import jax.numpy as jnp
import numpy as np
from jax import lax
from jax.experimental import pallas as pl
from jax.experimental.pallas import tpu as pltpu
from jax.sharding import PartitionSpec as P

HEAD = 128
THETA = 10000
NEG = -1e30
HIDDEN = 2 * NEG
LOG2E = 1.4426950408889634
MESH = pl.DeviceIdType.MESH
BF, F32 = jnp.bfloat16, jnp.float32

D = 6656
ROWS = 256
HEADS = 13
WIDTH = HEADS * HEAD
TILE = 512
QT = 10
OT = D // TILE
PAIRS = OT // 2
OU = 4
SLOTS = 3
LOCAL = 2 * QT
PIECE = QT + OU
REMOTE = LOCAL + 2 * PIECE
UNITS = REMOTE + 2 * OU
RING = 3
SUB = 4
PART = ROWS // SUB
STEPS = PART // 16
GROUPS = ((0, 1, 2, 3), (4, 5, 6, 7), (8, 9, 10, 11, 12))


def rope_tables():
    half = HEAD // 2
    place = np.arange(4 * ROWS, dtype=np.float32)[:, None]
    angle = place * np.power(np.float32(THETA), -np.arange(half, dtype=np.float32) / np.float32(half))
    cos, sin = np.cos(angle), np.sin(angle)
    cos = np.concatenate([np.concatenate([cos, cos], 1), np.ones((ROWS, HEAD))], 0)
    sin = np.concatenate([np.concatenate([-sin, sin], 1), np.zeros((ROWS, HEAD))], 0)
    return cos.astype(np.float32), sin.astype(np.float32)


def cols(n):
    return pl.ds(pl.multiple_of(n * TILE, TILE), TILE)


def rows_of(block):
    return pl.ds(pl.multiple_of(block * ROWS, ROWS), ROWS)


def pair(n):
    return pl.ds(pl.multiple_of(n * 2 * TILE, 2 * TILE), 2 * TILE)


def quarter(j):
    return pl.ds(pl.multiple_of(j * WIDTH, WIDTH), WIDTH)


def kernel(x, gain, wq, wk, wv, wo, cos_h, sin_h, y,
           a, qkv, seen, w, r_in, d_out, d_in, acc, raw, cos, sin, top_s, mix_s, gap_s,
           w_sem, x_sem, t_sem, swap_s, swap_r, link_s, link_r, pass_s, pass_r, d_s, d_r, rs_s, rs_r, l_s, l_r, y_sem):
    me = lax.axis_index("tp")
    c = lax.rem(me, 2)
    far = 1 - lax.div(me, 2)
    peer = me + 1 - 2 * c
    across = far * 2 + c
    diagonal = far * 2 + 1 - c

    def remote(src, dst, s, r, to):
        return pltpu.make_async_remote_copy(src_ref=src, dst_ref=dst, send_sem=s, recv_sem=r, device_id={"tp": to}, device_id_type=MESH)

    def issue(g):
        slot = lax.rem(g, SLOTS)
        in_piece = lax.rem(jnp.maximum(g - LOCAL, 0), PIECE)
        out = (g >= REMOTE) | ((g >= LOCAL) & (in_piece >= QT))
        t = jnp.where(g < LOCAL, lax.rem(g, QT), in_piece)
        u = jnp.where(g >= REMOTE, lax.rem(jnp.maximum(g - REMOTE, 0), OU), jnp.maximum(in_piece - QT, 0))
        project = jnp.logical_not(out)
        for i, ref in enumerate((wq, wk, wv)):

            @pl.when(project & (t >= 3 * i) & (t < 3 * i + 3))
            def _(i=i, ref=ref):
                for j in range(4):
                    pltpu.make_async_copy(ref.at[quarter(j), cols(lax.rem(t, 3))], w.at[slot, quarter(j)], w_sem.at[slot, j]).start()

        @pl.when(project & (t == QT - 1))
        def _():
            for j, ref in enumerate((wq, wk, wv, wv)):
                pltpu.make_async_copy(ref.at[:, pl.ds(3 * TILE, HEAD)], w.at[slot, :, pl.ds(j * HEAD, HEAD)], w_sem.at[slot, j]).start()

        for j in range(4):

            @pl.when(out & (g < UNITS) & (u * 4 + j < OT))
            def _(j=j):
                pltpu.make_async_copy(wo.at[:, cols(u * 4 + j)], w.at[slot, quarter(j)], w_sem.at[slot, j]).start()

    def fetched(slot, j):
        pltpu.make_async_copy(wo.at[:, pl.ds(0, TILE)], w.at[slot, quarter(j)], w_sem.at[slot, j]).wait()

    def part(block, s):
        return a.at[pl.ds(pl.multiple_of(block * ROWS + s * PART, PART), PART)]

    def swap(s):
        return remote(part(me, s), part(me, s), swap_s.at[s], swap_r.at[s], peer)

    def link(s):
        return remote(part(me, s), part(me, s), link_s.at[s], link_r.at[s], across)

    def passed(s):
        return remote(part(across, s), part(across, s), pass_s.at[s], pass_r.at[s], peer)

    def raw_link():
        return remote(x.at[pl.ds(0, PART)], part(me, 0), link_s.at[0], link_r.at[0], across)

    def pass_on(s):
        link(s).wait_recv()
        passed(s).start()

    def pass_first():
        raw_link().wait_recv()

        def step(i, _):
            norm(lambda: a[pl.ds(pl.multiple_of(across * ROWS + i * 16, 16), 16), :], across, i * 16)

        lax.fori_loop(0, STEPS, step, None)

    loads = [pltpu.make_async_copy(x.at[pl.ds(s * PART, PART)], r_in.at[pl.ds(s * PART, PART)], x_sem.at[s]) for s in range(SUB)]
    tables = [pltpu.make_async_copy(cos_h, cos, t_sem.at[0]), pltpu.make_async_copy(sin_h, sin, t_sem.at[1])]
    for copy in loads:
        copy.start()
    barrier = pltpu.get_barrier_semaphore()
    for to in (peer, across, diagonal):
        pl.semaphore_signal(barrier, inc=1, device_id={"tp": to}, device_id_type=MESH)

    def norm(get, block, at):
        wide = get().astype(F32)
        scale = lax.rsqrt(jnp.mean(wide * wide, -1, keepdims=True) + 1e-6)
        a[pl.ds(pl.multiple_of(block * ROWS + at, 16), 16), :] = (wide * scale * gain[...].reshape(1, D).astype(F32)).astype(BF)

    def send(s):
        swap(s).start()

        @pl.when((c == 0) & (s > 0))
        def _():
            link(s).start()

    def own(i, _):
        s = lax.div(i, STEPS)

        @pl.when(lax.rem(i, STEPS) == 0)
        def _():
            pltpu.make_async_copy(x.at[pl.ds(0, PART)], r_in.at[pl.ds(0, PART)], x_sem.at[s]).wait()

        norm(lambda: r_in[pl.ds(pl.multiple_of(i * 16, 16), 16), :], me, i * 16)

        @pl.when((lax.rem(i, STEPS) == 0) & (i > 0))
        def _():
            send(s - 1)

        @pl.when(i == STEPS)
        def _():
            issue(jnp.int32(0))

    pl.semaphore_wait(barrier, 3)

    @pl.when(c == 0)
    def _():
        raw_link().start()

    lax.fori_loop(0, SUB * STEPS, own, None)
    for copy in tables:
        copy.start()
    issue(jnp.int32(1))
    gap_s[...] = lax.broadcasted_iota(jnp.int32, (ROWS, ROWS), 1) - lax.broadcasted_iota(jnp.int32, (ROWS, ROWS), 0)
    send(SUB - 1)
    for copy in tables:
        copy.wait()

    def turn(t, block, at):
        for i in range(4):
            slot = jnp.where(t < QT - 1, lax.div(t, 3) * HEADS + lax.rem(t, 3) * 4 + i, min(i * HEADS + HEADS - 1, 3 * HEADS))
            plain = ((t >= 6) & (t < QT - 1)) | ((t == QT - 1) & (i >= 2))
            angles = pl.ds(pl.multiple_of(jnp.where(plain, 4, block) * ROWS, ROWS), ROWS)
            v = raw[at, :, pl.ds(i * HEAD, HEAD)].astype(F32)
            v = v * cos[angles, :] + pltpu.roll(v, HEAD // 2, 1) * sin[angles, :]
            qkv[slot, rows_of(block), :] = v.astype(BF)

    def project(g, t, block, before):
        issue(g + SLOTS - 1)
        slot = lax.rem(g, SLOTS)
        for j in range(4):
            fetched(slot, j)
        raw[lax.rem(t, 2)] = jnp.dot(a[rows_of(block), :], w[slot], preferred_element_type=F32).astype(BF)
        turn(*before)

    def local(i, _):
        t, block = lax.rem(i, QT), jnp.where(i < QT, me, peer)
        late = jnp.maximum(i - 1, 0)

        @pl.when(i == QT)
        def _():
            for s in range(SUB):
                swap(s).wait_recv()

        @pl.when((c == 1) & (i == 15))
        def _():
            for s in range(SUB):
                link(s).start()

        @pl.when((c == 0) & (i == 6))
        def _():
            pass_first()

        @pl.when((c == 0) & (i == 7))
        def _():
            passed(0).start()

        for s in range(1, SUB - 1):

            @pl.when((c == 0) & (i == 4 * s + 6))
            def _(s=s):
                pass_on(s)

        project(i, t, block, (lax.rem(late, QT), jnp.where(late < QT, me, peer), lax.rem(late, 2)))

    raw[...] = jnp.zeros_like(raw)
    lax.fori_loop(0, 2 * QT, local, None)
    turn(jnp.int32(QT - 1), peer, (QT - 1) % 2)

    @pl.when(c == 0)
    def _():
        pass_on(SUB - 1)

    def attend(block):
        e = HEAD**-0.5 * LOG2E
        top_s[...] = jnp.full(top_s.shape, NEG, F32)
        mix_s[...] = jnp.zeros(mix_s.shape, F32)
        ones = jnp.ones((8, ROWS), BF)

        def keys(j, _):
            ok = gap_s[...] >= (j - block) * ROWS
            for heads in GROUPS:
                scores = [
                    lax.dot_general(qkv[HEADS + h, rows_of(j), :], qkv[h, rows_of(block), :], (((1,), (1,)), ((), ())), preferred_element_type=F32)
                    for h in heads
                ]
                weights, keeps = [], []
                for h, s in zip(heads, scores):
                    s = jnp.where(ok, s, HIDDEN)
                    old = top_s[h : h + 1, :]
                    top = jnp.maximum(old, s.max(axis=0, keepdims=True))
                    top_s[h : h + 1, :] = top
                    weights.append(jnp.exp2((s - top) * e).astype(BF))
                    keeps.append(jnp.exp2((old - top) * e))
                for h, p, keep in zip(heads, weights, keeps):
                    values = jnp.concatenate([qkv[2 * HEADS + h, rows_of(j), :].T, ones], axis=0)
                    mix_s[h] = mix_s[h] * keep + jnp.dot(values, p, preferred_element_type=F32)

        lax.fori_loop(0, block + 1, keys, None)
        for h in range(HEADS):
            done = mix_s[h, :HEAD, :] * (1 / mix_s[h, HEAD : HEAD + 1, :])
            seen[rows_of(block), pl.ds(h * HEAD, HEAD)] = done.T.astype(BF)

    def output(base, block, k, tiles, put):
        slot = lax.rem(base + lax.div(k, 2), SLOTS)
        first = lax.rem(k, 2) * 2

        @pl.when(first == 0)
        def _():
            issue(base + lax.div(k, 2) + SLOTS - 1)

        for j in range(tiles):
            fetched(slot, first + j)
        for j in range(tiles):
            put(j, jnp.dot(seen[rows_of(block), :], w[slot, quarter(first + j), :], preferred_element_type=F32))

    def some(k, tiles):
        return pair(k) if tiles == 2 else pl.ds(PAIRS * 2 * TILE, TILE)

    mine = pl.ds(pl.multiple_of(c * 128, 128), 128)
    others = pl.ds(pl.multiple_of((1 - c) * 128, 128), 128)

    def exchange(q, tiles):
        slot, width = lax.rem(q, RING), pl.ds(0, tiles * TILE)
        return remote(d_out.at[slot, :, width], d_in.at[slot, :, width], d_s.at[slot], d_r.at[slot], peer)

    def sums(p):
        return pl.ds(pl.multiple_of(peer * ROWS + p * 128, 128), 128)

    def back(p, k, tiles):
        return remote(a.at[sums(p), some(k, tiles)], r_in.at[mine, some(k, tiles)], rs_s.at[p, k], rs_r.at[c, k], far * 2 + p)

    def add(p, k, tiles):
        q, width = p * (PAIRS + 1) + k, pl.ds(0, tiles * TILE)
        exchange(q, tiles).wait_recv()
        total = acc[lax.rem(k, 2), mine, width] + d_in[lax.rem(q, RING), :, width].astype(F32)
        a[sums(p), some(k, tiles)] = total.astype(BF)

    def finish(p):
        add(p, jnp.int32(PAIRS), 1)
        back(p, PAIRS, 1).start()

    def piece(p, _):
        block = far * 2 + p
        base = LOCAL + p * PIECE

        @pl.when(c != p)
        def _():
            for s in range(SUB):
                passed(s).wait_recv()

        def tiles(t, _):
            for s, i in ((0, 2), (1, 7)):

                @pl.when((c == 1) & (p == 0) & (t == i))
                def _(s=s):
                    pass_on(s)

            @pl.when((p == 1) & (t == 1))
            def _():
                finish(0)

            late = jnp.maximum(t - 1, 0)
            project(base + t, t, block, (late, block, lax.rem(late, 2)))

        lax.fori_loop(0, QT, tiles, None)
        turn(jnp.int32(QT - 1), block, (QT - 1) % 2)
        attend(block)

        @pl.when((c == 1) & (p == 0))
        def _():
            pass_on(2)

        def tiles_out(k, tiles):
            q, at = p * (PAIRS + 1) + k, lax.rem(k, 2)

            def put(j, value):
                acc[at, :, pl.ds(j * TILE, TILE)] = value

            output(base + QT, block, k, tiles, put)

            @pl.when(k >= 1)
            def _():
                add(p, k - 1, 2)

            @pl.when((q >= RING) & (lax.rem(q - RING, PAIRS + 1) < PAIRS))
            def _():
                exchange(q - RING, 2).wait_send()

            @pl.when((q >= RING) & (lax.rem(q - RING + PAIRS + 1, PAIRS + 1) == PAIRS))
            def _():
                exchange(q - RING, 1).wait_send()

            d_out[lax.rem(q, RING), :, pl.ds(0, tiles * TILE)] = acc[at, others, pl.ds(0, tiles * TILE)].astype(BF)

            @pl.when(k >= 1)
            def _():
                back(p, k - 1, 2).start()

            exchange(q, tiles).start()

        @pl.when(p == 1)
        def _():
            for s in range(SUB):
                swap(s).wait_send()
                link(s).wait_send()

        lax.fori_loop(0, PAIRS, lambda k, _: tiles_out(k, 2), None)
        tiles_out(jnp.int32(PAIRS), 1)

        @pl.when((c == 1) & (p == 0))
        def _():
            pass_on(SUB - 1)

    lax.fori_loop(0, 2, piece, None)
    for s in range(SUB):
        passed(s).wait_send()
    again = pltpu.make_async_copy(x, a.at[rows_of(diagonal)], x_sem.at[0])
    again.start()

    def own_chip(i, _):
        attend((1 - far) * 2 + i)

        @pl.when(i == 0)
        def _():
            finish(1)

    lax.fori_loop(0, 2, own_chip, None)
    for q in range(2 * (PAIRS + 1) - RING, 2 * (PAIRS + 1)):
        exchange(jnp.int32(q), 1 if q % (PAIRS + 1) == PAIRS else 2).wait_send()

    def give(k, tiles):
        return remote(a.at[rows_of(across), some(k, tiles)], a.at[rows_of(peer), some(k, tiles)], l_s.at[k], l_r.at[k], peer)

    def tiles_peer(k, tiles):
        def put(j, value):
            a[rows_of(across), pl.ds(pl.multiple_of(k * 2 * TILE + j * TILE, TILE), TILE)] = value.astype(BF)

        output(REMOTE, peer, k, tiles, put)

        @pl.when(k >= 1)
        def _():
            give(k - 1, 2).start()

    lax.fori_loop(0, PAIRS, lambda k, _: tiles_peer(k, 2), None)
    tiles_peer(jnp.int32(PAIRS), 1)

    def keep(k, tiles):
        return pltpu.make_async_copy(a.at[rows_of(diagonal), some(k, tiles)], y.at[:, some(k, tiles)], y_sem.at[k])

    again.wait()
    give(PAIRS, 1).start()

    def tiles_mine(k, tiles):
        def put(j, value):
            acc[0, :, pl.ds(j * TILE, TILE)] = value

        output(REMOTE + OU, me, k, tiles, put)
        here, width = some(k, tiles), pl.ds(0, tiles * TILE)
        remote(a.at[rows_of(across), here], a.at[rows_of(me), here], l_s.at[k], l_r.at[k], peer).wait_recv()
        for half in range(2):
            remote(a.at[sums(0), here], r_in.at[pl.ds(half * 128, 128), here], rs_s.at[0, k], rs_r.at[half, k], across).wait_recv()
        total = acc[0, :, width] + a[rows_of(me), here].astype(F32) + r_in[:, here].astype(F32)
        a[rows_of(diagonal), here] = (a[rows_of(diagonal), here].astype(F32) + total).astype(BF)

        @pl.when(k >= 1)
        def _():
            keep(k - 1, 2).start()

    lax.fori_loop(0, PAIRS, lambda k, _: tiles_mine(k, 2), None)
    tiles_mine(jnp.int32(PAIRS), 1)
    for k in range(PAIRS + 1):
        tiles = 2 if k < PAIRS else 1
        give(k, tiles).wait_send()
        for p in range(2):
            back(p, k, tiles).wait_send()
    keep(PAIRS, 1).start()
    for k in range(PAIRS + 1):
        keep(k, 2 if k < PAIRS else 1).wait()


def solution(mesh):
    tables = rope_tables()

    def step(x, gain, wq, wk, wv, wo):
        anywhere, vmem, dma = pl.BlockSpec(memory_space=pl.ANY), pltpu.VMEM, pltpu.SemaphoreType.DMA
        return pl.pallas_call(
            kernel,
            out_shape=jax.ShapeDtypeStruct((ROWS, D), BF),
            in_specs=[anywhere, pl.BlockSpec(memory_space=pltpu.VMEM)] + [anywhere] * 6,
            out_specs=anywhere,
            scratch_shapes=[
                vmem((4 * ROWS, D), BF),
                vmem((3 * HEADS + 1, 4 * ROWS, HEAD), BF),
                vmem((4 * ROWS, WIDTH), BF),
                vmem((SLOTS, D, TILE), BF),
                vmem((ROWS, D), BF),
                vmem((RING, 128, 2 * TILE), BF),
                vmem((RING, 128, 2 * TILE), BF),
                vmem((2, ROWS, 2 * TILE), F32),
                vmem((2, ROWS, TILE), BF),
                vmem((5 * ROWS, HEAD), F32),
                vmem((5 * ROWS, HEAD), F32),
                vmem((16, ROWS), F32),
                vmem((HEADS, HEAD + 8, ROWS), F32),
                vmem((ROWS, ROWS), jnp.int32),
                dma((SLOTS, 4)),
                dma((SUB,)),
                dma((2,)),
                dma((SUB,)),
                dma((SUB,)),
                dma((SUB,)),
                dma((SUB,)),
                dma((SUB,)),
                dma((SUB,)),
                dma((RING,)),
                dma((RING,)),
                dma((2, PAIRS + 1)),
                dma((2, PAIRS + 1)),
                dma((PAIRS + 1,)),
                dma((PAIRS + 1,)),
                dma((PAIRS + 1,)),
            ],
            compiler_params=pltpu.CompilerParams(collective_id=0, has_side_effects=True, vmem_limit_bytes=67_043_328),
            name="layer",
        )(x, gain, wq, wk, wv, wo, *(jnp.asarray(t) for t in tables))

    tokens, columns = P(("dp", "tp"), None), P(None, "tp")
    return jax.shard_map(
        step,
        mesh=mesh,
        in_specs=(tokens, P(None), columns, columns, columns, P("tp", None)),
        out_specs=tokens,
        check_vma=False,
    )
```

```python
import functools

import jax
import jax.numpy as jnp
import numpy as np
from jax import lax
from jax.experimental import pallas as pl
from jax.experimental.pallas import tpu as pltpu
from jax.sharding import PartitionSpec as P

HEAD = 128
THETA = 10000
NEG = -1e30
HIDDEN = 2 * NEG
LOG2E = 1.4426950408889634
MESH = pl.DeviceIdType.MESH
BF, F32 = jnp.bfloat16, jnp.float32

D = 6656
ROWS = 256
HEADS = 13
WIDTH = HEADS * HEAD
TILE = 512
QT = 10
OT = D // TILE
PAIRS = OT // 2
OU = 4
SLOTS = 3
LOCAL = 2 * QT
PIECE = QT + OU
REMOTE = LOCAL + 2 * PIECE
UNITS = REMOTE + 2 * OU
RING = 3
SUB = 4
PART = ROWS // SUB
STEPS = PART // 16
GROUPS = ((0, 1, 2, 3), (4, 5, 6, 7), (8, 9, 10, 11, 12))


def rope_tables():
    half = HEAD // 2
    place = np.arange(4 * ROWS, dtype=np.float32)[:, None]
    angle = place * np.power(np.float32(THETA), -np.arange(half, dtype=np.float32) / np.float32(half))
    cos, sin = np.cos(angle), np.sin(angle)
    cos = np.concatenate([np.concatenate([cos, cos], 1), np.ones((ROWS, HEAD))], 0)
    sin = np.concatenate([np.concatenate([-sin, sin], 1), np.zeros((ROWS, HEAD))], 0)
    return cos.astype(np.float32), sin.astype(np.float32)


def cols(n):
    return pl.ds(pl.multiple_of(n * TILE, TILE), TILE)


def rows_of(block):
    return pl.ds(pl.multiple_of(block * ROWS, ROWS), ROWS)


def pair(n):
    return pl.ds(pl.multiple_of(n * 2 * TILE, 2 * TILE), 2 * TILE)


def quarter(j):
    return pl.ds(pl.multiple_of(j * WIDTH, WIDTH), WIDTH)


def kernel(x, gain, wq, wk, wv, wo, cos_h, sin_h, y,
           a, qkv, seen, w, r_in, d_out, d_in, acc, raw, cos, sin, top_s, mix_s, gap_s,
           w_sem, x_sem, t_sem, swap_s, swap_r, link_s, link_r, pass_s, pass_r, d_s, d_r, rs_s, rs_r, l_s, l_r, y_sem):
    me = lax.axis_index("tp")
    c = lax.rem(me, 2)
    far = 1 - lax.div(me, 2)
    peer = me + 1 - 2 * c
    across = far * 2 + c
    diagonal = far * 2 + 1 - c

    def remote(src, dst, s, r, to):
        return pltpu.make_async_remote_copy(src_ref=src, dst_ref=dst, send_sem=s, recv_sem=r, device_id={"tp": to}, device_id_type=MESH)

    def issue(g):
        slot = lax.rem(g, SLOTS)
        in_piece = lax.rem(jnp.maximum(g - LOCAL, 0), PIECE)
        out = (g >= REMOTE) | ((g >= LOCAL) & (in_piece >= QT))
        t = jnp.where(g < LOCAL, lax.rem(g, QT), in_piece)
        u = jnp.where(g >= REMOTE, lax.rem(jnp.maximum(g - REMOTE, 0), OU), jnp.maximum(in_piece - QT, 0))
        project = jnp.logical_not(out)
        for i, ref in enumerate((wq, wk, wv)):

            @pl.when(project & (t >= 3 * i) & (t < 3 * i + 3))
            def _(i=i, ref=ref):
                for j in range(4):
                    pltpu.make_async_copy(ref.at[quarter(j), cols(lax.rem(t, 3))], w.at[slot, quarter(j)], w_sem.at[slot, j]).start()

        @pl.when(project & (t == QT - 1))
        def _():
            for j, ref in enumerate((wq, wk, wv, wv)):
                pltpu.make_async_copy(ref.at[:, pl.ds(3 * TILE, HEAD)], w.at[slot, :, pl.ds(j * HEAD, HEAD)], w_sem.at[slot, j]).start()

        for j in range(4):

            @pl.when(out & (g < UNITS) & (u * 4 + j < OT))
            def _(j=j):
                pltpu.make_async_copy(wo.at[:, cols(u * 4 + j)], w.at[slot, quarter(j)], w_sem.at[slot, j]).start()

    def fetched(slot, j):
        pltpu.make_async_copy(wo.at[:, pl.ds(0, TILE)], w.at[slot, quarter(j)], w_sem.at[slot, j]).wait()

    def part(block, s):
        return a.at[pl.ds(pl.multiple_of(block * ROWS + s * PART, PART), PART)]

    def swap(s):
        return remote(part(me, s), part(me, s), swap_s.at[s], swap_r.at[s], peer)

    def link(s):
        return remote(part(me, s), part(me, s), link_s.at[s], link_r.at[s], across)

    def passed(s):
        return remote(part(across, s), part(across, s), pass_s.at[s], pass_r.at[s], peer)

    def raw_link():
        return remote(x.at[pl.ds(0, PART)], part(me, 0), link_s.at[0], link_r.at[0], across)

    def pass_on(s):
        link(s).wait_recv()
        passed(s).start()

    def pass_first():
        raw_link().wait_recv()

        def step(i, _):
            norm(lambda: a[pl.ds(pl.multiple_of(across * ROWS + i * 16, 16), 16), :], across, i * 16)

        lax.fori_loop(0, STEPS, step, None)

    loads = [pltpu.make_async_copy(x.at[pl.ds(s * PART, PART)], r_in.at[pl.ds(s * PART, PART)], x_sem.at[s]) for s in range(SUB)]
    tables = [pltpu.make_async_copy(cos_h, cos, t_sem.at[0]), pltpu.make_async_copy(sin_h, sin, t_sem.at[1])]
    for copy in loads:
        copy.start()
    for copy in tables:
        copy.start()
    barrier = pltpu.get_barrier_semaphore()
    for to in (peer, across, diagonal):
        pl.semaphore_signal(barrier, inc=1, device_id={"tp": to}, device_id_type=MESH)

    def norm(get, block, at):
        wide = get().astype(F32)
        scale = lax.rsqrt(jnp.mean(wide * wide, -1, keepdims=True) + 1e-6)
        a[pl.ds(pl.multiple_of(block * ROWS + at, 16), 16), :] = (wide * scale * gain[...].reshape(1, D).astype(F32)).astype(BF)

    def send(s):
        swap(s).start()

        @pl.when((c == 0) & (s > 0))
        def _():
            link(s).start()

    def own(i, _):
        s = lax.div(i, STEPS)

        @pl.when(lax.rem(i, STEPS) == 0)
        def _():
            pltpu.make_async_copy(x.at[pl.ds(0, PART)], r_in.at[pl.ds(0, PART)], x_sem.at[s]).wait()

        norm(lambda: r_in[pl.ds(pl.multiple_of(i * 16, 16), 16), :], me, i * 16)

        @pl.when((lax.rem(i, STEPS) == 0) & (i > 0))
        def _():
            send(s - 1)

        for g, at in ((0, 1), (1, (SUB - 1) * STEPS + 1)):

            @pl.when(i == at)
            def _(g=g):
                issue(jnp.int32(g))

    pl.semaphore_wait(barrier, 3)

    @pl.when(c == 0)
    def _():
        raw_link().start()

    lax.fori_loop(0, SUB * STEPS, own, None)
    gap_s[...] = lax.broadcasted_iota(jnp.int32, (ROWS, ROWS), 1) - lax.broadcasted_iota(jnp.int32, (ROWS, ROWS), 0)
    send(SUB - 1)
    for copy in tables:
        copy.wait()

    def turn(t, block, at):
        for i in range(4):
            slot = jnp.where(t < QT - 1, lax.div(t, 3) * HEADS + lax.rem(t, 3) * 4 + i, min(i * HEADS + HEADS - 1, 3 * HEADS))
            plain = ((t >= 6) & (t < QT - 1)) | ((t == QT - 1) & (i >= 2))
            angles = pl.ds(pl.multiple_of(jnp.where(plain, 4, block) * ROWS, ROWS), ROWS)
            v = raw[at, :, pl.ds(i * HEAD, HEAD)].astype(F32)
            v = v * cos[angles, :] + pltpu.roll(v, HEAD // 2, 1) * sin[angles, :]
            qkv[slot, rows_of(block), :] = v.astype(BF)

    def project(g, t, block, before):
        issue(g + SLOTS - 1)
        slot = lax.rem(g, SLOTS)
        for j in range(4):
            fetched(slot, j)
        raw[lax.rem(t, 2)] = jnp.dot(a[rows_of(block), :], w[slot], preferred_element_type=F32).astype(BF)
        turn(*before)

    def local(i, _):
        t, block = lax.rem(i, QT), jnp.where(i < QT, me, peer)
        late = jnp.maximum(i - 1, 0)

        @pl.when(i == QT)
        def _():
            for s in range(SUB):
                swap(s).wait_recv()

        @pl.when((c == 1) & (i == 15))
        def _():
            for s in range(SUB):
                link(s).start()

        @pl.when((c == 0) & (i == 6))
        def _():
            pass_first()

        @pl.when((c == 0) & (i == 7))
        def _():
            passed(0).start()

        for s, at in ((1, 10), (2, 14), (3, 19)):

            @pl.when((c == 0) & (i == at))
            def _(s=s):
                pass_on(s)

        project(i, t, block, (lax.rem(late, QT), jnp.where(late < QT, me, peer), lax.rem(late, 2)))

    raw[...] = jnp.zeros_like(raw)
    lax.fori_loop(0, 2 * QT, local, None)
    turn(jnp.int32(QT - 1), peer, (QT - 1) % 2)


    def attend(block):
        e = HEAD**-0.5 * LOG2E
        top_s[...] = jnp.full(top_s.shape, NEG, F32)
        mix_s[...] = jnp.zeros(mix_s.shape, F32)
        ones = jnp.ones((8, ROWS), BF)

        def keys(j, _):
            ok = gap_s[...] >= (j - block) * ROWS
            for heads in GROUPS:
                scores = [
                    lax.dot_general(qkv[HEADS + h, rows_of(j), :], qkv[h, rows_of(block), :], (((1,), (1,)), ((), ())), preferred_element_type=F32)
                    for h in heads
                ]
                weights, keeps = [], []
                for h, s in zip(heads, scores):
                    s = jnp.where(ok, s, HIDDEN)
                    old = top_s[h : h + 1, :]
                    top = jnp.maximum(old, s.max(axis=0, keepdims=True))
                    top_s[h : h + 1, :] = top
                    weights.append(jnp.exp2((s - top) * e).astype(BF))
                    keeps.append(jnp.exp2((old - top) * e))
                for h, p, keep in zip(heads, weights, keeps):
                    values = jnp.concatenate([qkv[2 * HEADS + h, rows_of(j), :].T, ones], axis=0)
                    mix_s[h] = mix_s[h] * keep + jnp.dot(values, p, preferred_element_type=F32)

        lax.fori_loop(0, block + 1, keys, None)
        for h in range(HEADS):
            done = mix_s[h, :HEAD, :] * (1 / mix_s[h, HEAD : HEAD + 1, :])
            seen[rows_of(block), pl.ds(h * HEAD, HEAD)] = done.T.astype(BF)

    def output(base, block, k, tiles, put):
        slot = lax.rem(base + lax.div(k, 2), SLOTS)
        first = lax.rem(k, 2) * 2

        @pl.when(first == 0)
        def _():
            issue(base + lax.div(k, 2) + SLOTS - 1)

        for j in range(tiles):
            fetched(slot, first + j)
        for j in range(tiles):
            put(j, jnp.dot(seen[rows_of(block), :], w[slot, quarter(first + j), :], preferred_element_type=F32))

    def some(k, tiles):
        return pair(k) if tiles == 2 else pl.ds(PAIRS * 2 * TILE, TILE)

    mine = pl.ds(pl.multiple_of(c * 128, 128), 128)
    others = pl.ds(pl.multiple_of((1 - c) * 128, 128), 128)

    def exchange(q, tiles):
        slot, width = lax.rem(q, RING), pl.ds(0, tiles * TILE)
        return remote(d_out.at[slot, :, width], d_in.at[slot, :, width], d_s.at[slot], d_r.at[slot], peer)

    def sums(p):
        return pl.ds(pl.multiple_of(peer * ROWS + p * 128, 128), 128)

    def back(p, k, tiles):
        return remote(a.at[sums(p), some(k, tiles)], r_in.at[mine, some(k, tiles)], rs_s.at[p, k], rs_r.at[c, k], far * 2 + p)

    def add(p, k, tiles):
        q, width = p * (PAIRS + 1) + k, pl.ds(0, tiles * TILE)
        exchange(q, tiles).wait_recv()
        total = acc[lax.rem(k, 2), mine, width] + d_in[lax.rem(q, RING), :, width].astype(F32)
        a[sums(p), some(k, tiles)] = total.astype(BF)

    def finish(p):
        add(p, jnp.int32(PAIRS), 1)
        back(p, PAIRS, 1).start()

    def piece(p, _):
        block = far * 2 + p
        base = LOCAL + p * PIECE

        @pl.when(c != p)
        def _():
            for s in range(SUB):
                passed(s).wait_recv()

        def tiles(t, _):
            for s, i in ((0, 2), (1, 7)):

                @pl.when((c == 1) & (p == 0) & (t == i))
                def _(s=s):
                    pass_on(s)

            @pl.when((p == 1) & (t == 1))
            def _():
                finish(0)

            late = jnp.maximum(t - 1, 0)
            project(base + t, t, block, (late, block, lax.rem(late, 2)))

        lax.fori_loop(0, QT, tiles, None)
        turn(jnp.int32(QT - 1), block, (QT - 1) % 2)
        attend(block)

        @pl.when((c == 1) & (p == 0))
        def _():
            pass_on(2)

        def tiles_out(k, tiles):
            q, at = p * (PAIRS + 1) + k, lax.rem(k, 2)

            def put(j, value):
                acc[at, :, pl.ds(j * TILE, TILE)] = value

            output(base + QT, block, k, tiles, put)

            @pl.when(k >= 1)
            def _():
                add(p, k - 1, 2)

            @pl.when((q >= RING) & (lax.rem(q - RING, PAIRS + 1) < PAIRS))
            def _():
                exchange(q - RING, 2).wait_send()

            @pl.when((q >= RING) & (lax.rem(q - RING + PAIRS + 1, PAIRS + 1) == PAIRS))
            def _():
                exchange(q - RING, 1).wait_send()

            d_out[lax.rem(q, RING), :, pl.ds(0, tiles * TILE)] = acc[at, others, pl.ds(0, tiles * TILE)].astype(BF)

            @pl.when(k >= 1)
            def _():
                back(p, k - 1, 2).start()

            exchange(q, tiles).start()

        @pl.when(p == 1)
        def _():
            for s in range(SUB):
                swap(s).wait_send()
                link(s).wait_send()

        def pairs_out(k, _):
            @pl.when((c == 1) & (p == 0) & (k == PAIRS - 1))
            def _():
                pass_on(SUB - 1)

            tiles_out(k, 2)

        lax.fori_loop(0, PAIRS, pairs_out, None)
        tiles_out(jnp.int32(PAIRS), 1)

    lax.fori_loop(0, 2, piece, None)
    for s in range(SUB):
        passed(s).wait_send()
    again = pltpu.make_async_copy(x, a.at[rows_of(diagonal)], x_sem.at[0])
    again.start()

    def own_chip(i, _):
        attend((1 - far) * 2 + i)

        @pl.when(i == 0)
        def _():
            finish(1)

    lax.fori_loop(0, 2, own_chip, None)
    for q in range(2 * (PAIRS + 1) - RING, 2 * (PAIRS + 1)):
        exchange(jnp.int32(q), 1 if q % (PAIRS + 1) == PAIRS else 2).wait_send()

    def give(k, tiles):
        return remote(a.at[rows_of(across), some(k, tiles)], a.at[rows_of(peer), some(k, tiles)], l_s.at[k], l_r.at[k], peer)

    def tiles_peer(k, tiles):
        def put(j, value):
            a[rows_of(across), pl.ds(pl.multiple_of(k * 2 * TILE + j * TILE, TILE), TILE)] = value.astype(BF)

        output(REMOTE, peer, k, tiles, put)

        @pl.when(k >= 1)
        def _():
            give(k - 1, 2).start()

    lax.fori_loop(0, PAIRS, lambda k, _: tiles_peer(k, 2), None)
    tiles_peer(jnp.int32(PAIRS), 1)

    def keep(k, tiles):
        return pltpu.make_async_copy(a.at[rows_of(diagonal), some(k, tiles)], y.at[:, some(k, tiles)], y_sem.at[k])

    again.wait()
    give(PAIRS, 1).start()

    def tiles_mine(k, tiles):
        def put(j, value):
            acc[0, :, pl.ds(j * TILE, TILE)] = value

        output(REMOTE + OU, me, k, tiles, put)
        here, width = some(k, tiles), pl.ds(0, tiles * TILE)
        remote(a.at[rows_of(across), here], a.at[rows_of(me), here], l_s.at[k], l_r.at[k], peer).wait_recv()
        for half in range(2):
            remote(a.at[sums(0), here], r_in.at[pl.ds(half * 128, 128), here], rs_s.at[0, k], rs_r.at[half, k], across).wait_recv()
        total = acc[0, :, width] + a[rows_of(me), here].astype(F32) + r_in[:, here].astype(F32)
        a[rows_of(diagonal), here] = (a[rows_of(diagonal), here].astype(F32) + total).astype(BF)

        @pl.when(k >= 1)
        def _():
            keep(k - 1, 2).start()

    lax.fori_loop(0, PAIRS, lambda k, _: tiles_mine(k, 2), None)
    tiles_mine(jnp.int32(PAIRS), 1)
    for k in range(PAIRS + 1):
        tiles = 2 if k < PAIRS else 1
        give(k, tiles).wait_send()
        for p in range(2):
            back(p, k, tiles).wait_send()
    keep(PAIRS, 1).start()
    for k in range(PAIRS + 1):
        keep(k, 2 if k < PAIRS else 1).wait()


def solution(mesh):
    tables = rope_tables()

    def step(x, gain, wq, wk, wv, wo):
        anywhere, vmem, dma = pl.BlockSpec(memory_space=pl.ANY), pltpu.VMEM, pltpu.SemaphoreType.DMA
        return pl.pallas_call(
            kernel,
            out_shape=jax.ShapeDtypeStruct((ROWS, D), BF),
            in_specs=[anywhere, pl.BlockSpec(memory_space=pltpu.VMEM)] + [anywhere] * 6,
            out_specs=anywhere,
            scratch_shapes=[
                vmem((4 * ROWS, D), BF),
                vmem((3 * HEADS + 1, 4 * ROWS, HEAD), BF),
                vmem((4 * ROWS, WIDTH), BF),
                vmem((SLOTS, D, TILE), BF),
                vmem((ROWS, D), BF),
                vmem((RING, 128, 2 * TILE), BF),
                vmem((RING, 128, 2 * TILE), BF),
                vmem((2, ROWS, 2 * TILE), F32),
                vmem((2, ROWS, TILE), BF),
                vmem((5 * ROWS, HEAD), F32),
                vmem((5 * ROWS, HEAD), F32),
                vmem((16, ROWS), F32),
                vmem((HEADS, HEAD + 8, ROWS), F32),
                vmem((ROWS, ROWS), jnp.int32),
                dma((SLOTS, 4)),
                dma((SUB,)),
                dma((2,)),
                dma((SUB,)),
                dma((SUB,)),
                dma((SUB,)),
                dma((SUB,)),
                dma((SUB,)),
                dma((SUB,)),
                dma((RING,)),
                dma((RING,)),
                dma((2, PAIRS + 1)),
                dma((2, PAIRS + 1)),
                dma((PAIRS + 1,)),
                dma((PAIRS + 1,)),
                dma((PAIRS + 1,)),
            ],
            compiler_params=pltpu.CompilerParams(collective_id=0, has_side_effects=True, vmem_limit_bytes=67_043_328),
            name="layer",
        )(x, gain, wq, wk, wv, wo, *(jnp.asarray(t) for t in tables))

    tokens, columns = P(("dp", "tp"), None), P(None, "tp")
    return jax.shard_map(
        step,
        mesh=mesh,
        in_specs=(tokens, P(None), columns, columns, columns, P("tp", None)),
        out_specs=tokens,
        check_vma=False,
    )
```

```python
import functools

import jax
import jax.numpy as jnp
import numpy as np
from jax import lax
from jax.experimental import pallas as pl
from jax.experimental.pallas import tpu as pltpu
from jax.sharding import PartitionSpec as P

HEAD = 128
THETA = 10000
NEG = -1e30
HIDDEN = 2 * NEG
LOG2E = 1.4426950408889634
MESH = pl.DeviceIdType.MESH
BF, F32 = jnp.bfloat16, jnp.float32

D = 6656
ROWS = 256
HEADS = 13
WIDTH = HEADS * HEAD
TILE = 512
QT = 10
OT = D // TILE
PAIRS = OT // 2
OU = 4
SLOTS = 3
LOCAL = 2 * QT
PIECE = QT + OU
REMOTE = LOCAL + 2 * PIECE
UNITS = REMOTE + 2 * OU
RING = 3
SUB = 4
PART = ROWS // SUB
STEPS = PART // 16
GROUPS = ((0, 1, 2, 3), (4, 5, 6, 7), (8, 9, 10, 11, 12))


def rope_tables():
    half = HEAD // 2
    place = np.arange(4 * ROWS, dtype=np.float32)[:, None]
    angle = place * np.power(np.float32(THETA), -np.arange(half, dtype=np.float32) / np.float32(half))
    cos, sin = np.cos(angle), np.sin(angle)
    cos = np.concatenate([np.concatenate([cos, cos], 1), np.ones((ROWS, HEAD))], 0)
    sin = np.concatenate([np.concatenate([-sin, sin], 1), np.zeros((ROWS, HEAD))], 0)
    return cos.astype(np.float32), sin.astype(np.float32)


def cols(n):
    return pl.ds(pl.multiple_of(n * TILE, TILE), TILE)


def rows_of(block):
    return pl.ds(pl.multiple_of(block * ROWS, ROWS), ROWS)


def pair(n):
    return pl.ds(pl.multiple_of(n * 2 * TILE, 2 * TILE), 2 * TILE)


def quarter(j):
    return pl.ds(pl.multiple_of(j * WIDTH, WIDTH), WIDTH)


def kernel(x, gain, wq, wk, wv, wo, cos_h, sin_h, y,
           a, qkv, seen, w, r_in, d_out, d_in, acc, raw, cos, sin, top_s, mix_s, gap_s,
           w_sem, x_sem, t_sem, swap_s, swap_r, link_s, link_r, pass_s, pass_r, d_s, d_r, rs_s, rs_r, l_s, l_r):
    me = lax.axis_index("tp")
    c = lax.rem(me, 2)
    far = 1 - lax.div(me, 2)
    peer = me + 1 - 2 * c
    across = far * 2 + c
    diagonal = far * 2 + 1 - c

    def remote(src, dst, s, r, to):
        return pltpu.make_async_remote_copy(src_ref=src, dst_ref=dst, send_sem=s, recv_sem=r, device_id={"tp": to}, device_id_type=MESH)

    def issue(g):
        slot = lax.rem(g, SLOTS)
        in_piece = lax.rem(jnp.maximum(g - LOCAL, 0), PIECE)
        out = (g >= REMOTE) | ((g >= LOCAL) & (in_piece >= QT))
        t = jnp.where(g < LOCAL, lax.rem(g, QT), in_piece)
        u = jnp.where(g >= REMOTE, lax.rem(jnp.maximum(g - REMOTE, 0), OU), jnp.maximum(in_piece - QT, 0))
        project = jnp.logical_not(out)
        for i, ref in enumerate((wq, wk, wv)):

            @pl.when(project & (t >= 3 * i) & (t < 3 * i + 3))
            def _(i=i, ref=ref):
                for j in range(4):
                    pltpu.make_async_copy(ref.at[quarter(j), cols(lax.rem(t, 3))], w.at[slot, quarter(j)], w_sem.at[slot, j]).start()

        @pl.when(project & (t == QT - 1))
        def _():
            for j, ref in enumerate((wq, wk, wv, wv)):
                pltpu.make_async_copy(ref.at[:, pl.ds(3 * TILE, HEAD)], w.at[slot, :, pl.ds(j * HEAD, HEAD)], w_sem.at[slot, j]).start()

        for j in range(4):

            @pl.when(out & (g < UNITS) & (u * 4 + j < OT))
            def _(j=j):
                pltpu.make_async_copy(wo.at[:, cols(u * 4 + j)], w.at[slot, quarter(j)], w_sem.at[slot, j]).start()

    def fetched(slot, j):
        pltpu.make_async_copy(wo.at[:, pl.ds(0, TILE)], w.at[slot, quarter(j)], w_sem.at[slot, j]).wait()

    def part(block, s):
        return a.at[pl.ds(pl.multiple_of(block * ROWS + s * PART, PART), PART)]

    def swap(s):
        return remote(part(me, s), part(me, s), swap_s.at[s], swap_r.at[s], peer)

    def link(s):
        return remote(part(me, s), part(me, s), link_s.at[s], link_r.at[s], across)

    def passed(s):
        return remote(part(across, s), part(across, s), pass_s.at[s], pass_r.at[s], peer)

    def pass_on(s):
        link(s).wait_recv()
        passed(s).start()

    loads = [pltpu.make_async_copy(x.at[pl.ds(s * PART, PART)], r_in.at[pl.ds(s * PART, PART)], x_sem.at[s]) for s in range(SUB)]
    tables = [pltpu.make_async_copy(cos_h, cos, t_sem.at[0]), pltpu.make_async_copy(sin_h, sin, t_sem.at[1])]
    for copy in loads:
        copy.start()
    for copy in tables:
        copy.start()
    barrier = pltpu.get_barrier_semaphore()
    for to in (peer, across, diagonal):
        pl.semaphore_signal(barrier, inc=1, device_id={"tp": to}, device_id_type=MESH)

    def send(s):
        swap(s).start()

        @pl.when(c == 0)
        def _():
            link(s).start()

    def own(i, _):
        s = lax.div(i, STEPS)

        @pl.when(lax.rem(i, STEPS) == 0)
        def _():
            pltpu.make_async_copy(x.at[pl.ds(0, PART)], r_in.at[pl.ds(0, PART)], x_sem.at[s]).wait()

        wide = r_in[pl.ds(pl.multiple_of(i * 16, 16), 16), :].astype(F32)
        scale = lax.rsqrt(jnp.mean(wide * wide, -1, keepdims=True) + 1e-6)
        a[pl.ds(pl.multiple_of(me * ROWS + i * 16, 16), 16), :] = (wide * scale * gain[...].reshape(1, D).astype(F32)).astype(BF)

        for g, at in ((0, 1), (1, (SUB - 1) * STEPS + 1)):

            @pl.when(i == at)
            def _(g=g):
                issue(jnp.int32(g))

    lax.fori_loop(0, 2 * STEPS, own, None)
    pl.semaphore_wait(barrier, 3)
    send(0)

    def own_and_send(i, _):
        own(i, _)

        @pl.when(lax.rem(i, STEPS) == 0)
        def _():
            send(lax.div(i, STEPS) - 1)

    lax.fori_loop(2 * STEPS, SUB * STEPS, own_and_send, None)
    gap_s[...] = lax.broadcasted_iota(jnp.int32, (ROWS, ROWS), 1) - lax.broadcasted_iota(jnp.int32, (ROWS, ROWS), 0)
    send(SUB - 1)
    for copy in tables:
        copy.wait()

    def turn(t, block, at):
        for i in range(4):
            slot = jnp.where(t < QT - 1, lax.div(t, 3) * HEADS + lax.rem(t, 3) * 4 + i, min(i * HEADS + HEADS - 1, 3 * HEADS))
            plain = ((t >= 6) & (t < QT - 1)) | ((t == QT - 1) & (i >= 2))
            angles = pl.ds(pl.multiple_of(jnp.where(plain, 4, block) * ROWS, ROWS), ROWS)
            v = raw[at, :, pl.ds(i * HEAD, HEAD)].astype(F32)
            v = v * cos[angles, :] + pltpu.roll(v, HEAD // 2, 1) * sin[angles, :]
            qkv[slot, rows_of(block), :] = v.astype(BF)

    def project(g, t, block, before):
        issue(g + SLOTS - 1)
        slot = lax.rem(g, SLOTS)
        for j in range(4):
            fetched(slot, j)
        raw[lax.rem(t, 2)] = jnp.dot(a[rows_of(block), :], w[slot], preferred_element_type=F32).astype(BF)
        turn(*before)

    def local(i, _):
        t, block = lax.rem(i, QT), jnp.where(i < QT, me, peer)
        late = jnp.maximum(i - 1, 0)

        @pl.when(i == QT)
        def _():
            for s in range(SUB):
                swap(s).wait_recv()

        @pl.when((c == 1) & (i == 15))
        def _():
            for s in range(SUB):
                link(s).start()

        for s, at in ((0, 6), (1, 10), (2, 14), (3, 19)):

            @pl.when((c == 0) & (i == at))
            def _(s=s):
                pass_on(s)

        project(i, t, block, (lax.rem(late, QT), jnp.where(late < QT, me, peer), lax.rem(late, 2)))

    raw[...] = jnp.zeros_like(raw)
    lax.fori_loop(0, 2 * QT, local, None)
    turn(jnp.int32(QT - 1), peer, (QT - 1) % 2)


    def attend(block):
        e = HEAD**-0.5 * LOG2E
        top_s[...] = jnp.full(top_s.shape, NEG, F32)
        mix_s[...] = jnp.zeros(mix_s.shape, F32)
        ones = jnp.ones((8, ROWS), BF)

        def keys(j, _):
            ok = gap_s[...] >= (j - block) * ROWS
            for heads in GROUPS:
                scores = [
                    lax.dot_general(qkv[HEADS + h, rows_of(j), :], qkv[h, rows_of(block), :], (((1,), (1,)), ((), ())), preferred_element_type=F32)
                    for h in heads
                ]
                weights, keeps = [], []
                for h, s in zip(heads, scores):
                    s = jnp.where(ok, s, HIDDEN)
                    old = top_s[h : h + 1, :]
                    top = jnp.maximum(old, s.max(axis=0, keepdims=True))
                    top_s[h : h + 1, :] = top
                    weights.append(jnp.exp2((s - top) * e).astype(BF))
                    keeps.append(jnp.exp2((old - top) * e))
                for h, p, keep in zip(heads, weights, keeps):
                    values = jnp.concatenate([qkv[2 * HEADS + h, rows_of(j), :].T, ones], axis=0)
                    mix_s[h] = mix_s[h] * keep + jnp.dot(values, p, preferred_element_type=F32)

        lax.fori_loop(0, block + 1, keys, None)
        for h in range(HEADS):
            done = mix_s[h, :HEAD, :] * (1 / mix_s[h, HEAD : HEAD + 1, :])
            seen[rows_of(block), pl.ds(h * HEAD, HEAD)] = done.T.astype(BF)

    def output(base, block, k, tiles, put):
        slot = lax.rem(base + lax.div(k, 2), SLOTS)
        first = lax.rem(k, 2) * 2

        @pl.when(first == 0)
        def _():
            issue(base + lax.div(k, 2) + SLOTS - 1)

        for j in range(tiles):
            fetched(slot, first + j)
        for j in range(tiles):
            put(j, jnp.dot(seen[rows_of(block), :], w[slot, quarter(first + j), :], preferred_element_type=F32))

    def some(k, tiles):
        return pair(k) if tiles == 2 else pl.ds(PAIRS * 2 * TILE, TILE)

    mine = pl.ds(pl.multiple_of(c * 128, 128), 128)
    others = pl.ds(pl.multiple_of((1 - c) * 128, 128), 128)

    def exchange(q, tiles):
        slot, width = lax.rem(q, RING), pl.ds(0, tiles * TILE)
        return remote(d_out.at[slot, :, width], d_in.at[slot, :, width], d_s.at[slot], d_r.at[slot], peer)

    def sums(p):
        return pl.ds(pl.multiple_of(peer * ROWS + p * 128, 128), 128)

    def back(p, k, tiles):
        return remote(a.at[sums(p), some(k, tiles)], r_in.at[mine, some(k, tiles)], rs_s.at[p, k], rs_r.at[c, k], far * 2 + p)

    def add(p, k, tiles):
        q, width = p * (PAIRS + 1) + k, pl.ds(0, tiles * TILE)
        exchange(q, tiles).wait_recv()
        total = acc[lax.rem(k, 2), mine, width] + d_in[lax.rem(q, RING), :, width].astype(F32)
        a[sums(p), some(k, tiles)] = total.astype(BF)

    def finish(p):
        add(p, jnp.int32(PAIRS), 1)
        back(p, PAIRS, 1).start()

    def piece(p, _):
        block = far * 2 + p
        base = LOCAL + p * PIECE

        @pl.when(c != p)
        def _():
            for s in range(SUB):
                passed(s).wait_recv()

        def tiles(t, _):
            for s, i in ((0, 2), (1, 7)):

                @pl.when((c == 1) & (p == 0) & (t == i))
                def _(s=s):
                    pass_on(s)

            @pl.when((p == 1) & (t == 1))
            def _():
                finish(0)

            late = jnp.maximum(t - 1, 0)
            project(base + t, t, block, (late, block, lax.rem(late, 2)))

        lax.fori_loop(0, QT, tiles, None)
        turn(jnp.int32(QT - 1), block, (QT - 1) % 2)
        attend(block)

        @pl.when((c == 1) & (p == 0))
        def _():
            pass_on(2)

        def tiles_out(k, tiles):
            q, at = p * (PAIRS + 1) + k, lax.rem(k, 2)

            def put(j, value):
                acc[at, :, pl.ds(j * TILE, TILE)] = value

            output(base + QT, block, k, tiles, put)

            @pl.when(k >= 1)
            def _():
                add(p, k - 1, 2)

            @pl.when((q >= RING) & (lax.rem(q - RING, PAIRS + 1) < PAIRS))
            def _():
                exchange(q - RING, 2).wait_send()

            @pl.when((q >= RING) & (lax.rem(q - RING + PAIRS + 1, PAIRS + 1) == PAIRS))
            def _():
                exchange(q - RING, 1).wait_send()

            d_out[lax.rem(q, RING), :, pl.ds(0, tiles * TILE)] = acc[at, others, pl.ds(0, tiles * TILE)].astype(BF)

            @pl.when(k >= 1)
            def _():
                back(p, k - 1, 2).start()

            exchange(q, tiles).start()

        @pl.when(p == 1)
        def _():
            for s in range(SUB):
                swap(s).wait_send()
                link(s).wait_send()

        def pairs_out(k, _):
            @pl.when((c == 1) & (p == 0) & (k == PAIRS - 1))
            def _():
                pass_on(SUB - 1)

            tiles_out(k, 2)

        lax.fori_loop(0, PAIRS, pairs_out, None)
        tiles_out(jnp.int32(PAIRS), 1)

    lax.fori_loop(0, 2, piece, None)
    for s in range(SUB):
        passed(s).wait_send()
    again = pltpu.make_async_copy(x, a.at[rows_of(diagonal)], x_sem.at[0])
    again.start()

    def own_chip(i, _):
        attend((1 - far) * 2 + i)

        @pl.when(i == 0)
        def _():
            finish(1)

    lax.fori_loop(0, 2, own_chip, None)
    for q in range(2 * (PAIRS + 1) - RING, 2 * (PAIRS + 1)):
        exchange(jnp.int32(q), 1 if q % (PAIRS + 1) == PAIRS else 2).wait_send()

    def give(k, tiles):
        return remote(a.at[rows_of(across), some(k, tiles)], a.at[rows_of(peer), some(k, tiles)], l_s.at[k], l_r.at[k], peer)

    def tiles_peer(k, tiles):
        def put(j, value):
            a[rows_of(across), pl.ds(pl.multiple_of(k * 2 * TILE + j * TILE, TILE), TILE)] = value.astype(BF)

        output(REMOTE, peer, k, tiles, put)

        @pl.when(k >= 1)
        def _():
            give(k - 1, 2).start()

    lax.fori_loop(0, PAIRS, lambda k, _: tiles_peer(k, 2), None)
    tiles_peer(jnp.int32(PAIRS), 1)

    again.wait()
    give(PAIRS, 1).start()

    def tiles_mine(k, tiles):
        def put(j, value):
            acc[0, :, pl.ds(j * TILE, TILE)] = value

        output(REMOTE + OU, me, k, tiles, put)
        here, width = some(k, tiles), pl.ds(0, tiles * TILE)
        remote(a.at[rows_of(across), here], a.at[rows_of(me), here], l_s.at[k], l_r.at[k], peer).wait_recv()
        for half in range(2):
            remote(a.at[sums(0), here], r_in.at[pl.ds(half * 128, 128), here], rs_s.at[0, k], rs_r.at[half, k], across).wait_recv()
        total = acc[0, :, width] + a[rows_of(me), here].astype(F32) + r_in[:, here].astype(F32)
        y[:, here] = (a[rows_of(diagonal), here].astype(F32) + total).astype(BF)

    lax.fori_loop(0, PAIRS, lambda k, _: tiles_mine(k, 2), None)
    tiles_mine(jnp.int32(PAIRS), 1)
    for k in range(PAIRS + 1):
        tiles = 2 if k < PAIRS else 1
        give(k, tiles).wait_send()
        for p in range(2):
            back(p, k, tiles).wait_send()


def solution(mesh):
    tables = rope_tables()

    def step(x, gain, wq, wk, wv, wo):
        anywhere, vmem, dma = pl.BlockSpec(memory_space=pl.ANY), pltpu.VMEM, pltpu.SemaphoreType.DMA
        return pl.pallas_call(
            kernel,
            out_shape=pltpu.VMEM((ROWS, D), BF),
            in_specs=[anywhere, pl.BlockSpec(memory_space=pltpu.VMEM)] + [anywhere] * 6,
            out_specs=pl.BlockSpec(memory_space=pltpu.VMEM),
            scratch_shapes=[
                vmem((4 * ROWS, D), BF),
                vmem((3 * HEADS + 1, 4 * ROWS, HEAD), BF),
                vmem((4 * ROWS, WIDTH), BF),
                vmem((SLOTS, D, TILE), BF),
                vmem((ROWS, D), BF),
                vmem((RING, 128, 2 * TILE), BF),
                vmem((RING, 128, 2 * TILE), BF),
                vmem((2, ROWS, 2 * TILE), F32),
                vmem((2, ROWS, TILE), BF),
                vmem((5 * ROWS, HEAD), F32),
                vmem((5 * ROWS, HEAD), F32),
                vmem((16, ROWS), F32),
                vmem((HEADS, HEAD + 8, ROWS), F32),
                vmem((ROWS, ROWS), jnp.int32),
                dma((SLOTS, 4)),
                dma((SUB,)),
                dma((2,)),
                dma((SUB,)),
                dma((SUB,)),
                dma((SUB,)),
                dma((SUB,)),
                dma((SUB,)),
                dma((SUB,)),
                dma((RING,)),
                dma((RING,)),
                dma((2, PAIRS + 1)),
                dma((2, PAIRS + 1)),
                dma((PAIRS + 1,)),
                dma((PAIRS + 1,)),
            ],
            compiler_params=pltpu.CompilerParams(collective_id=0, has_side_effects=True, vmem_limit_bytes=63_000_000),
            name="layer",
        )(x, gain, wq, wk, wv, wo, *(jnp.asarray(t) for t in tables))

    tokens, columns = P(("dp", "tp"), None), P(None, "tp")
    return jax.shard_map(
        step,
        mesh=mesh,
        in_specs=(tokens, P(None), columns, columns, columns, P("tp", None)),
        out_specs=tokens,
        check_vma=False,
    )
```

```python
import functools

import jax
import jax.numpy as jnp
import numpy as np
from jax import lax
from jax.experimental import pallas as pl
from jax.experimental.pallas import tpu as pltpu
from jax.sharding import PartitionSpec as P

HEAD = 128
THETA = 10000
NEG = -1e30
HIDDEN = 2 * NEG
LOG2E = 1.4426950408889634
MESH = pl.DeviceIdType.MESH
BF, F32 = jnp.bfloat16, jnp.float32

D = 6656
ROWS = 256
HEADS = 13
WIDTH = HEADS * HEAD
TILE = 512
QT = 10
OT = D // TILE
PAIRS = OT // 2
OU = 4
SLOTS = 3
LOCAL = 2 * QT
PIECE = QT + OU
REMOTE = LOCAL + 2 * PIECE
UNITS = REMOTE + 2 * OU
RING = 3
SUB = 4
PART = ROWS // SUB
STEPS = PART // 16
GROUPS = ((0, 1, 2, 3), (4, 5, 6, 7), (8, 9, 10, 11, 12))


def rope_tables():
    half = HEAD // 2
    place = np.arange(4 * ROWS, dtype=np.float32)[:, None]
    angle = place * np.power(np.float32(THETA), -np.arange(half, dtype=np.float32) / np.float32(half))
    cos, sin = np.cos(angle), np.sin(angle)
    cos = np.concatenate([np.concatenate([cos, cos], 1), np.ones((ROWS, HEAD))], 0)
    sin = np.concatenate([np.concatenate([-sin, sin], 1), np.zeros((ROWS, HEAD))], 0)
    return cos.astype(np.float32), sin.astype(np.float32)


def cols(n):
    return pl.ds(pl.multiple_of(n * TILE, TILE), TILE)


def rows_of(block):
    return pl.ds(pl.multiple_of(block * ROWS, ROWS), ROWS)


def pair(n):
    return pl.ds(pl.multiple_of(n * 2 * TILE, 2 * TILE), 2 * TILE)


def quarter(j):
    return pl.ds(pl.multiple_of(j * WIDTH, WIDTH), WIDTH)


def kernel(x, gain, wq, wk, wv, wo, cos_h, sin_h, y,
           a, qkv, seen, w, r_in, d_out, d_in, acc, raw, cos, sin, top_s, mix_s,
           w_sem, x_sem, t_sem, swap_s, swap_r, link_s, link_r, pass_s, pass_r, d_s, d_r, rs_s, rs_r, l_s, l_r):
    me = lax.axis_index("tp")
    c = lax.rem(me, 2)
    far = 1 - lax.div(me, 2)
    peer = me + 1 - 2 * c
    across = far * 2 + c
    diagonal = far * 2 + 1 - c

    def remote(src, dst, s, r, to):
        return pltpu.make_async_remote_copy(src_ref=src, dst_ref=dst, send_sem=s, recv_sem=r, device_id={"tp": to}, device_id_type=MESH)

    def issue(g):
        slot = lax.rem(g, SLOTS)
        in_piece = lax.rem(jnp.maximum(g - LOCAL, 0), PIECE)
        out = (g >= REMOTE) | ((g >= LOCAL) & (in_piece >= QT))
        t = jnp.where(g < LOCAL, lax.rem(g, QT), in_piece)
        u = jnp.where(g >= REMOTE, lax.rem(jnp.maximum(g - REMOTE, 0), OU), jnp.maximum(in_piece - QT, 0))
        project = jnp.logical_not(out)
        for i, ref in enumerate((wq, wk, wv)):

            @pl.when(project & (t >= 3 * i) & (t < 3 * i + 3))
            def _(i=i, ref=ref):
                for j in range(4):
                    pltpu.make_async_copy(ref.at[quarter(j), cols(lax.rem(t, 3))], w.at[slot, quarter(j)], w_sem.at[slot, j]).start()

        @pl.when(project & (t == QT - 1))
        def _():
            for j, ref in enumerate((wq, wk, wv, wv)):
                pltpu.make_async_copy(ref.at[:, pl.ds(3 * TILE, HEAD)], w.at[slot, :, pl.ds(j * HEAD, HEAD)], w_sem.at[slot, j]).start()

        for j in range(4):

            @pl.when(out & (g < UNITS) & (u * 4 + j < OT))
            def _(j=j):
                pltpu.make_async_copy(wo.at[:, cols(u * 4 + j)], w.at[slot, quarter(j)], w_sem.at[slot, j]).start()

    def fetched(slot, j):
        pltpu.make_async_copy(wo.at[:, pl.ds(0, TILE)], w.at[slot, quarter(j)], w_sem.at[slot, j]).wait()

    def part(block, s):
        return a.at[pl.ds(pl.multiple_of(block * ROWS + s * PART, PART), PART)]

    def swap(s):
        return remote(part(me, s), part(me, s), swap_s.at[s], swap_r.at[s], peer)

    def link(s):
        return remote(part(me, s), part(me, s), link_s.at[s], link_r.at[s], across)

    def passed(s):
        return remote(part(across, s), part(across, s), pass_s.at[s], pass_r.at[s], peer)

    def pass_on(s):
        link(s).wait_recv()
        passed(s).start()

    loads = [pltpu.make_async_copy(x.at[pl.ds(s * PART, PART)], r_in.at[pl.ds(s * PART, PART)], x_sem.at[s]) for s in range(SUB)]
    tables = [pltpu.make_async_copy(cos_h, cos, t_sem.at[0]), pltpu.make_async_copy(sin_h, sin, t_sem.at[1])]
    for copy in loads:
        copy.start()
    for copy in tables:
        copy.start()
    barrier = pltpu.get_barrier_semaphore()
    for to in (peer, across, diagonal):
        pl.semaphore_signal(barrier, inc=1, device_id={"tp": to}, device_id_type=MESH)

    def send(s):
        swap(s).start()

        @pl.when(c == 0)
        def _():
            link(s).start()

    def own(i, _):
        s = lax.div(i, STEPS)

        @pl.when(lax.rem(i, STEPS) == 0)
        def _():
            pltpu.make_async_copy(x.at[pl.ds(0, PART)], r_in.at[pl.ds(0, PART)], x_sem.at[s]).wait()

        wide = r_in[pl.ds(pl.multiple_of(i * 16, 16), 16), :].astype(F32)
        scale = lax.rsqrt(jnp.mean(wide * wide, -1, keepdims=True) + 1e-6)
        a[pl.ds(pl.multiple_of(me * ROWS + i * 16, 16), 16), :] = (wide * scale * gain[...].reshape(1, D).astype(F32)).astype(BF)

        for g, at in ((0, 1), (1, (SUB - 1) * STEPS + 1)):

            @pl.when(i == at)
            def _(g=g):
                issue(jnp.int32(g))

    lax.fori_loop(0, 2 * STEPS, own, None)
    pl.semaphore_wait(barrier, 3)
    send(0)

    def own_and_send(i, _):
        own(i, _)

        @pl.when(lax.rem(i, STEPS) == 0)
        def _():
            send(lax.div(i, STEPS) - 1)

    lax.fori_loop(2 * STEPS, SUB * STEPS, own_and_send, None)
    send(SUB - 1)
    for copy in tables:
        copy.wait()

    def turn(t, block, at):
        for i in range(4):
            slot = jnp.where(t < QT - 1, lax.div(t, 3) * HEADS + lax.rem(t, 3) * 4 + i, min(i * HEADS + HEADS - 1, 3 * HEADS))
            plain = ((t >= 6) & (t < QT - 1)) | ((t == QT - 1) & (i >= 2))
            angles = pl.ds(pl.multiple_of(jnp.where(plain, 4, block) * ROWS, ROWS), ROWS)
            v = raw[at, :, pl.ds(i * HEAD, HEAD)].astype(F32)
            v = v * cos[angles, :] + pltpu.roll(v, HEAD // 2, 1) * sin[angles, :]
            qkv[slot, rows_of(block), :] = v.astype(BF)

    def project(g, t, block, before):
        issue(g + SLOTS - 1)
        slot = lax.rem(g, SLOTS)
        for j in range(4):
            fetched(slot, j)
        raw[lax.rem(t, 2)] = jnp.dot(a[rows_of(block), :], w[slot], preferred_element_type=F32).astype(BF)
        turn(*before)

    def local(i, _):
        t, block = lax.rem(i, QT), jnp.where(i < QT, me, peer)
        late = jnp.maximum(i - 1, 0)

        @pl.when(i == QT)
        def _():
            for s in range(SUB):
                swap(s).wait_recv()

        @pl.when((c == 1) & (i == 15))
        def _():
            for s in range(SUB):
                link(s).start()

        for s, at in ((0, 6), (1, 10), (2, 14), (3, 19)):

            @pl.when((c == 0) & (i == at))
            def _(s=s):
                pass_on(s)

        project(i, t, block, (lax.rem(late, QT), jnp.where(late < QT, me, peer), lax.rem(late, 2)))

    raw[...] = jnp.zeros_like(raw)
    lax.fori_loop(0, 2 * QT, local, None)
    turn(jnp.int32(QT - 1), peer, (QT - 1) % 2)


    def attend(block):
        e = HEAD**-0.5 * LOG2E
        top_s[...] = jnp.full(top_s.shape, NEG, F32)
        mix_s[...] = jnp.zeros(mix_s.shape, F32)
        ones = jnp.ones((8, ROWS), BF)

        def keys(j, masked):

            def score(heads):
                return [
                    lax.dot_general(qkv[HEADS + h, rows_of(j), :], qkv[h, rows_of(block), :], (((1,), (1,)), ((), ())), preferred_element_type=F32)
                    for h in heads
                ]

            ahead = score(GROUPS[0])
            for at, heads in enumerate(GROUPS):
                scores = ahead
                if at + 1 < len(GROUPS):
                    ahead = score(GROUPS[at + 1])
                weights, keeps = [], []
                for h, s in zip(heads, scores):
                    if masked:
                        s = jnp.where(lax.broadcasted_iota(jnp.int32, s.shape, 1) >= lax.broadcasted_iota(jnp.int32, s.shape, 0), s, HIDDEN)
                    old = top_s[h : h + 1, :]
                    top = jnp.maximum(old, s.max(axis=0, keepdims=True))
                    top_s[h : h + 1, :] = top
                    weights.append(jnp.exp2((s - top) * e).astype(BF))
                    keeps.append(jnp.exp2((old - top) * e))
                for h, p, keep in zip(heads, weights, keeps):
                    values = jnp.concatenate([qkv[2 * HEADS + h, rows_of(j), :].T, ones], axis=0)
                    mix_s[h] = mix_s[h] * keep + jnp.dot(values, p, preferred_element_type=F32)

        lax.fori_loop(0, block, lambda j, _: keys(j, False), None)
        keys(block, True)
        for h in range(HEADS):
            done = mix_s[h, :HEAD, :] * (1 / mix_s[h, HEAD : HEAD + 1, :])
            seen[rows_of(block), pl.ds(h * HEAD, HEAD)] = done.T.astype(BF)

    def output(base, block, k, tiles, put):
        slot = lax.rem(base + lax.div(k, 2), SLOTS)
        first = lax.rem(k, 2) * 2

        @pl.when(first == 0)
        def _():
            issue(base + lax.div(k, 2) + SLOTS - 1)

        for j in range(tiles):
            fetched(slot, first + j)
        for j in range(tiles):
            put(j, jnp.dot(seen[rows_of(block), :], w[slot, quarter(first + j), :], preferred_element_type=F32))

    def some(k, tiles):
        return pair(k) if tiles == 2 else pl.ds(PAIRS * 2 * TILE, TILE)

    mine = pl.ds(pl.multiple_of(c * 128, 128), 128)
    others = pl.ds(pl.multiple_of((1 - c) * 128, 128), 128)

    def exchange(q, tiles):
        slot, width = lax.rem(q, RING), pl.ds(0, tiles * TILE)
        return remote(d_out.at[slot, :, width], d_in.at[slot, :, width], d_s.at[slot], d_r.at[slot], peer)

    def sums(p):
        return pl.ds(pl.multiple_of(peer * ROWS + p * 128, 128), 128)

    def back(p, k, tiles):
        return remote(a.at[sums(p), some(k, tiles)], r_in.at[mine, some(k, tiles)], rs_s.at[p, k], rs_r.at[c, k], far * 2 + p)

    def add(p, k, tiles):
        q, width = p * (PAIRS + 1) + k, pl.ds(0, tiles * TILE)
        exchange(q, tiles).wait_recv()
        total = acc[lax.rem(k, 2), mine, width] + d_in[lax.rem(q, RING), :, width].astype(F32)
        a[sums(p), some(k, tiles)] = total.astype(BF)

    def finish(p):
        add(p, jnp.int32(PAIRS), 1)
        back(p, PAIRS, 1).start()

    def piece(p, _):
        block = far * 2 + p
        base = LOCAL + p * PIECE

        @pl.when(c != p)
        def _():
            for s in range(SUB):
                passed(s).wait_recv()

        def tiles(t, _):
            for s, i in ((0, 2), (1, 7)):

                @pl.when((c == 1) & (p == 0) & (t == i))
                def _(s=s):
                    pass_on(s)

            @pl.when((p == 1) & (t == 1))
            def _():
                finish(0)

            late = jnp.maximum(t - 1, 0)
            project(base + t, t, block, (late, block, lax.rem(late, 2)))

        lax.fori_loop(0, QT, tiles, None)
        turn(jnp.int32(QT - 1), block, (QT - 1) % 2)
        attend(block)

        @pl.when((c == 1) & (p == 0))
        def _():
            pass_on(2)

        def tiles_out(k, tiles):
            q, at = p * (PAIRS + 1) + k, lax.rem(k, 2)

            def put(j, value):
                acc[at, :, pl.ds(j * TILE, TILE)] = value

            output(base + QT, block, k, tiles, put)

            @pl.when(k >= 1)
            def _():
                add(p, k - 1, 2)

            @pl.when((q >= RING) & (lax.rem(q - RING, PAIRS + 1) < PAIRS))
            def _():
                exchange(q - RING, 2).wait_send()

            @pl.when((q >= RING) & (lax.rem(q - RING + PAIRS + 1, PAIRS + 1) == PAIRS))
            def _():
                exchange(q - RING, 1).wait_send()

            d_out[lax.rem(q, RING), :, pl.ds(0, tiles * TILE)] = acc[at, others, pl.ds(0, tiles * TILE)].astype(BF)

            @pl.when(k >= 1)
            def _():
                back(p, k - 1, 2).start()

            exchange(q, tiles).start()

        @pl.when(p == 1)
        def _():
            for s in range(SUB):
                swap(s).wait_send()
                link(s).wait_send()

        def pairs_out(k, _):
            @pl.when((c == 1) & (p == 0) & (k == PAIRS - 1))
            def _():
                pass_on(SUB - 1)

            tiles_out(k, 2)

        lax.fori_loop(0, PAIRS, pairs_out, None)
        tiles_out(jnp.int32(PAIRS), 1)

    lax.fori_loop(0, 2, piece, None)
    for s in range(SUB):
        passed(s).wait_send()
    again = pltpu.make_async_copy(x, a.at[rows_of(diagonal)], x_sem.at[0])
    again.start()

    def own_chip(i, _):
        attend((1 - far) * 2 + i)

        @pl.when(i == 0)
        def _():
            finish(1)

    lax.fori_loop(0, 2, own_chip, None)
    for q in range(2 * (PAIRS + 1) - RING, 2 * (PAIRS + 1)):
        exchange(jnp.int32(q), 1 if q % (PAIRS + 1) == PAIRS else 2).wait_send()

    def give(k, tiles):
        return remote(a.at[rows_of(across), some(k, tiles)], a.at[rows_of(peer), some(k, tiles)], l_s.at[k], l_r.at[k], peer)

    def tiles_peer(k, tiles):
        def put(j, value):
            a[rows_of(across), pl.ds(pl.multiple_of(k * 2 * TILE + j * TILE, TILE), TILE)] = value.astype(BF)

        output(REMOTE, peer, k, tiles, put)

        @pl.when(k >= 1)
        def _():
            give(k - 1, 2).start()

    lax.fori_loop(0, PAIRS, lambda k, _: tiles_peer(k, 2), None)
    tiles_peer(jnp.int32(PAIRS), 1)

    again.wait()
    give(PAIRS, 1).start()

    def tiles_mine(k, tiles):
        def put(j, value):
            acc[0, :, pl.ds(j * TILE, TILE)] = value

        output(REMOTE + OU, me, k, tiles, put)
        here, width = some(k, tiles), pl.ds(0, tiles * TILE)
        remote(a.at[rows_of(across), here], a.at[rows_of(me), here], l_s.at[k], l_r.at[k], peer).wait_recv()
        for half in range(2):
            remote(a.at[sums(0), here], r_in.at[pl.ds(half * 128, 128), here], rs_s.at[0, k], rs_r.at[half, k], across).wait_recv()
        total = acc[0, :, width] + a[rows_of(me), here].astype(F32) + r_in[:, here].astype(F32)
        y[:, here] = (a[rows_of(diagonal), here].astype(F32) + total).astype(BF)

    lax.fori_loop(0, PAIRS, lambda k, _: tiles_mine(k, 2), None)
    tiles_mine(jnp.int32(PAIRS), 1)
    for k in range(PAIRS + 1):
        tiles = 2 if k < PAIRS else 1
        give(k, tiles).wait_send()
        for p in range(2):
            back(p, k, tiles).wait_send()


def solution(mesh):
    tables = rope_tables()

    def step(x, gain, wq, wk, wv, wo):
        anywhere, vmem, dma = pl.BlockSpec(memory_space=pl.ANY), pltpu.VMEM, pltpu.SemaphoreType.DMA
        return pl.pallas_call(
            kernel,
            out_shape=pltpu.VMEM((ROWS, D), BF),
            in_specs=[anywhere, pl.BlockSpec(memory_space=pltpu.VMEM)] + [anywhere] * 6,
            out_specs=pl.BlockSpec(memory_space=pltpu.VMEM),
            scratch_shapes=[
                vmem((4 * ROWS, D), BF),
                vmem((3 * HEADS + 1, 4 * ROWS, HEAD), BF),
                vmem((4 * ROWS, WIDTH), BF),
                vmem((SLOTS, D, TILE), BF),
                vmem((ROWS, D), BF),
                vmem((RING, 128, 2 * TILE), BF),
                vmem((RING, 128, 2 * TILE), BF),
                vmem((2, ROWS, 2 * TILE), F32),
                vmem((2, ROWS, TILE), BF),
                vmem((5 * ROWS, HEAD), F32),
                vmem((5 * ROWS, HEAD), F32),
                vmem((16, ROWS), F32),
                vmem((HEADS, HEAD + 8, ROWS), F32),
                dma((SLOTS, 4)),
                dma((SUB,)),
                dma((2,)),
                dma((SUB,)),
                dma((SUB,)),
                dma((SUB,)),
                dma((SUB,)),
                dma((SUB,)),
                dma((SUB,)),
                dma((RING,)),
                dma((RING,)),
                dma((2, PAIRS + 1)),
                dma((2, PAIRS + 1)),
                dma((PAIRS + 1,)),
                dma((PAIRS + 1,)),
            ],
            compiler_params=pltpu.CompilerParams(collective_id=0, has_side_effects=True, vmem_limit_bytes=63_600_000),
            name="layer",
        )(x, gain, wq, wk, wv, wo, *(jnp.asarray(t) for t in tables))

    tokens, columns = P(("dp", "tp"), None), P(None, "tp")
    return jax.shard_map(
        step,
        mesh=mesh,
        in_specs=(tokens, P(None), columns, columns, columns, P("tp", None)),
        out_specs=tokens,
        check_vma=False,
    )
```

```python
import functools

import jax
import jax.numpy as jnp
import numpy as np
from jax import lax
from jax.experimental import pallas as pl
from jax.experimental.pallas import tpu as pltpu
from jax.sharding import PartitionSpec as P

HEAD = 128
THETA = 10000
NEG = -1e30
HIDDEN = 2 * NEG
LOG2E = 1.4426950408889634
MESH = pl.DeviceIdType.MESH
BF, F32 = jnp.bfloat16, jnp.float32

D = 6656
ROWS = 256
HEADS = 13
WIDTH = HEADS * HEAD
TILE = 512
QT = 10
OT = D // TILE
PAIRS = OT // 2
OU = 4
SLOTS = 3
LATER = 2
LOCAL = 2 * QT - LATER
PIECE = QT + OU
LATE = LOCAL + 2 * PIECE
REMOTE = LATE + LATER
UNITS = REMOTE + 2 * OU
RING = 3
SUB = 4
PART = ROWS // SUB
STEPS = PART // 16
GROUPS = ((0, 1, 2, 3), (4, 5, 6, 7), (8, 9, 10, 11, 12))


def rope_tables():
    half = HEAD // 2
    place = np.arange(4 * ROWS, dtype=np.float32)[:, None]
    angle = place * np.power(np.float32(THETA), -np.arange(half, dtype=np.float32) / np.float32(half))
    cos, sin = np.cos(angle), np.sin(angle)
    cos = np.concatenate([np.concatenate([cos, cos], 1), np.ones((ROWS, HEAD))], 0)
    sin = np.concatenate([np.concatenate([-sin, sin], 1), np.zeros((ROWS, HEAD))], 0)
    return cos.astype(np.float32), sin.astype(np.float32)


def cols(n):
    return pl.ds(pl.multiple_of(n * TILE, TILE), TILE)


def rows_of(block):
    return pl.ds(pl.multiple_of(block * ROWS, ROWS), ROWS)


def pair(n):
    return pl.ds(pl.multiple_of(n * 2 * TILE, 2 * TILE), 2 * TILE)


def quarter(j):
    return pl.ds(pl.multiple_of(j * WIDTH, WIDTH), WIDTH)


def own_tile(i):
    return jnp.where(i < QT, i, i - QT + LATER)


def kernel(x, gain_h, wq, wk, wv, wo, cos_h, sin_h, y,
           gain, a, qkv, seen, w, r_in, d_out, d_in, acc, raw, cos, sin, top_s, mix_s,
           w_sem, x_sem, t_sem, swap_s, swap_r, link_s, link_r, pass_s, pass_r, d_s, d_r, rs_s, rs_r, l_s, l_r):
    me = lax.axis_index("tp")
    c = lax.rem(me, 2)
    far = 1 - lax.div(me, 2)
    peer = me + 1 - 2 * c
    across = far * 2 + c
    diagonal = far * 2 + 1 - c

    def remote(src, dst, s, r, to):
        return pltpu.make_async_remote_copy(src_ref=src, dst_ref=dst, send_sem=s, recv_sem=r, device_id={"tp": to}, device_id_type=MESH)

    def issue(g):
        slot = lax.rem(g, SLOTS)
        in_piece = lax.rem(jnp.maximum(g - LOCAL, 0), PIECE)
        out = (g >= REMOTE) | ((g >= LOCAL) & (g < LATE) & (in_piece >= QT))
        t = jnp.where(g < LOCAL, own_tile(g), jnp.where(g < LATE, in_piece, g - LATE))
        u = jnp.where(g >= REMOTE, lax.rem(jnp.maximum(g - REMOTE, 0), OU), jnp.maximum(in_piece - QT, 0))
        project = jnp.logical_not(out)
        for i, ref in enumerate((wq, wk, wv)):

            @pl.when(project & (t >= 3 * i) & (t < 3 * i + 3))
            def _(i=i, ref=ref):
                for j in range(4):
                    pltpu.make_async_copy(ref.at[quarter(j), cols(lax.rem(t, 3))], w.at[slot, quarter(j)], w_sem.at[slot, j]).start()

        @pl.when(project & (t == QT - 1))
        def _():
            for j, ref in enumerate((wq, wk, wv, wv)):
                pltpu.make_async_copy(ref.at[:, pl.ds(3 * TILE, HEAD)], w.at[slot, :, pl.ds(j * HEAD, HEAD)], w_sem.at[slot, j]).start()

        for j in range(4):

            @pl.when(out & (g < UNITS) & (u * 4 + j < OT))
            def _(j=j):
                pltpu.make_async_copy(wo.at[:, cols(u * 4 + j)], w.at[slot, quarter(j)], w_sem.at[slot, j]).start()

    def fetched(slot, j):
        pltpu.make_async_copy(wo.at[:, pl.ds(0, TILE)], w.at[slot, quarter(j)], w_sem.at[slot, j]).wait()

    def part(block, s):
        return a.at[pl.ds(pl.multiple_of(block * ROWS + s * PART, PART), PART)]

    def swap(s):
        return remote(part(me, s), part(me, s), swap_s.at[s], swap_r.at[s], peer)

    def link(s):
        return remote(part(me, s), part(me, s), link_s.at[s], link_r.at[s], across)

    def passed(s):
        return remote(part(across, s), part(across, s), pass_s.at[s], pass_r.at[s], peer)

    def raw_link():
        return remote(x.at[pl.ds(0, PART)], part(me, 0), link_s.at[0], link_r.at[0], across)

    def pass_on(s):
        link(s).wait_recv()
        passed(s).start()

    loads = [pltpu.make_async_copy(x.at[pl.ds(s * PART, PART)], r_in.at[pl.ds(s * PART, PART)], x_sem.at[s]) for s in range(SUB)]
    tables = [pltpu.make_async_copy(cos_h, cos, t_sem.at[0]), pltpu.make_async_copy(sin_h, sin, t_sem.at[1])]
    gains = pltpu.make_async_copy(gain_h, gain, t_sem.at[2])
    barrier = pltpu.get_barrier_semaphore()
    for to in (peer, across, diagonal):
        pl.semaphore_signal(barrier, inc=1, device_id={"tp": to}, device_id_type=MESH)
    gains.start()
    for copy in loads:
        copy.start()
    for copy in tables:
        copy.start()

    @pl.when(far == 0)
    def _():
        pl.semaphore_wait(barrier, 3)

        @pl.when(c == 0)
        def _():
            raw_link().start()

    def norm(get, block, at):
        wide = get().astype(F32)
        scale = lax.rsqrt(jnp.mean(wide * wide, -1, keepdims=True) + 1e-6)
        a[pl.ds(pl.multiple_of(block * ROWS + at, 16), 16), :] = (wide * scale * gain[...].reshape(1, D).astype(F32)).astype(BF)

    def send(s):
        swap(s).start()

        @pl.when((c == 0) & ((s > 0) | (far == 1)))
        def _():
            link(s).start()

    def own(i, _):
        s = lax.div(i, STEPS)

        @pl.when(lax.rem(i, STEPS) == 0)
        def _():
            pltpu.make_async_copy(x.at[pl.ds(0, PART)], r_in.at[pl.ds(0, PART)], x_sem.at[s]).wait()

        norm(lambda: r_in[pl.ds(pl.multiple_of(i * 16, 16), 16), :], me, i * 16)

        for g, at in ((0, 1), (1, (SUB - 1) * STEPS + 1)):

            @pl.when(i == at)
            def _(g=g):
                issue(jnp.int32(g))

    gains.wait()
    lax.fori_loop(0, 2 * STEPS, own, None)

    @pl.when(far == 1)
    def _():
        pl.semaphore_wait(barrier, 3)

    send(0)

    def own_and_send(i, _):
        own(i, _)

        @pl.when(lax.rem(i, STEPS) == 0)
        def _():
            send(lax.div(i, STEPS) - 1)

    lax.fori_loop(2 * STEPS, SUB * STEPS, own_and_send, None)
    send(SUB - 1)
    for copy in tables:
        copy.wait()

    def turn(t, block, at):
        for i in range(4):
            slot = jnp.where(t < QT - 1, lax.div(t, 3) * HEADS + lax.rem(t, 3) * 4 + i, min(i * HEADS + HEADS - 1, 3 * HEADS))
            plain = ((t >= 6) & (t < QT - 1)) | ((t == QT - 1) & (i >= 2))
            angles = pl.ds(pl.multiple_of(jnp.where(plain, 4, block) * ROWS, ROWS), ROWS)
            v = raw[at, :, pl.ds(i * HEAD, HEAD)].astype(F32)
            v = v * cos[angles, :] + pltpu.roll(v, HEAD // 2, 1) * sin[angles, :]
            qkv[slot, rows_of(block), :] = v.astype(BF)

    def project(g, t, block, here, before):
        issue(g + SLOTS - 1)
        slot = lax.rem(g, SLOTS)
        for j in range(4):
            fetched(slot, j)
        raw[here] = jnp.dot(a[rows_of(block), :], w[slot], preferred_element_type=F32).astype(BF)
        turn(*before)

    def local(i, _):
        block = jnp.where(i < QT, me, peer)
        late = jnp.maximum(i - 1, 0)

        @pl.when(i == QT)
        def _():
            for s in range(SUB):
                swap(s).wait_recv()

        @pl.when((c == 1) & (i == 15))
        def _():
            for s in range(SUB):
                link(s).start()

        @pl.when((c == 0) & (far == 1) & (i == 6))
        def _():
            link(0).wait_recv()

            def step(n, _):
                norm(lambda: a[pl.ds(pl.multiple_of(across * ROWS + n * 16, 16), 16), :], across, n * 16)

            lax.fori_loop(0, STEPS, step, None)

        @pl.when((c == 0) & (far == 1) & (i == 7))
        def _():
            passed(0).start()

        @pl.when((c == 0) & (far == 0) & (i == 6))
        def _():
            pass_on(0)

        for s, at in ((1, 10), (2, 14), (3, 17)):

            @pl.when((c == 0) & (i == at))
            def _(s=s):
                pass_on(s)

        project(i, own_tile(i), block, lax.rem(i, 2), (own_tile(late), jnp.where(late < QT, me, peer), lax.rem(late, 2)))

    raw[...] = jnp.zeros_like(raw)
    lax.fori_loop(0, LOCAL, local, None)
    turn(jnp.int32(QT - 1), peer, (LOCAL - 1) % 2)


    def attend(block):
        e = HEAD**-0.5 * LOG2E
        top_s[...] = jnp.full(top_s.shape, NEG, F32)
        mix_s[...] = jnp.zeros(mix_s.shape, F32)
        ones = jnp.ones((8, ROWS), BF)

        def keys(j, masked):

            def score(heads):
                return [
                    lax.dot_general(qkv[HEADS + h, rows_of(j), :], qkv[h, rows_of(block), :], (((1,), (1,)), ((), ())), preferred_element_type=F32)
                    for h in heads
                ]

            ahead = score(GROUPS[0])
            for at, heads in enumerate(GROUPS):
                scores = ahead
                if at + 1 < len(GROUPS):
                    ahead = score(GROUPS[at + 1])
                weights, keeps = [], []
                for h, s in zip(heads, scores):
                    if masked:
                        s = jnp.where(lax.broadcasted_iota(jnp.int32, s.shape, 1) >= lax.broadcasted_iota(jnp.int32, s.shape, 0), s, HIDDEN)
                    old = top_s[h : h + 1, :]
                    top = jnp.maximum(old, s.max(axis=0, keepdims=True))
                    top_s[h : h + 1, :] = top
                    weights.append(jnp.exp2((s - top) * e).astype(BF))
                    keeps.append(jnp.exp2((old - top) * e))
                for h, p, keep in zip(heads, weights, keeps):
                    values = jnp.concatenate([qkv[2 * HEADS + h, rows_of(j), :].T, ones], axis=0)
                    mix_s[h] = mix_s[h] * keep + jnp.dot(values, p, preferred_element_type=F32)

        lax.fori_loop(0, block, lambda j, _: keys(j, False), None)
        keys(block, True)
        for h in range(HEADS):
            done = mix_s[h, :HEAD, :] * (1 / mix_s[h, HEAD : HEAD + 1, :])
            seen[rows_of(block), pl.ds(h * HEAD, HEAD)] = done.T.astype(BF)

    def output(base, block, k, tiles, put):
        slot = lax.rem(base + lax.div(k, 2), SLOTS)
        first = lax.rem(k, 2) * 2

        @pl.when(first == 0)
        def _():
            issue(base + lax.div(k, 2) + SLOTS - 1)

        for j in range(tiles):
            fetched(slot, first + j)
        for j in range(tiles):
            put(j, jnp.dot(seen[rows_of(block), :], w[slot, quarter(first + j), :], preferred_element_type=F32))

    def some(k, tiles):
        return pair(k) if tiles == 2 else pl.ds(PAIRS * 2 * TILE, TILE)

    mine = pl.ds(pl.multiple_of(c * 128, 128), 128)
    others = pl.ds(pl.multiple_of((1 - c) * 128, 128), 128)

    def exchange(q, tiles):
        slot, width = lax.rem(q, RING), pl.ds(0, tiles * TILE)
        return remote(d_out.at[slot, :, width], d_in.at[slot, :, width], d_s.at[slot], d_r.at[slot], peer)

    def sums(p):
        return pl.ds(pl.multiple_of(p * 128, 128), 128)

    def back(p, k, tiles):
        return remote(y.at[sums(p), some(k, tiles)], r_in.at[mine, some(k, tiles)], rs_s.at[p, k], rs_r.at[c, k], far * 2 + p)

    def add(p, k, tiles):
        q, width = p * (PAIRS + 1) + k, pl.ds(0, tiles * TILE)
        exchange(q, tiles).wait_recv()
        total = acc[lax.rem(k, 2), mine, width] + d_in[lax.rem(q, RING), :, width].astype(F32)
        y[sums(p), some(k, tiles)] = total.astype(BF)

    def finish(p):
        add(p, jnp.int32(PAIRS), 1)
        back(p, PAIRS, 1).start()

    def piece(p, _):
        block = far * 2 + p
        base = LOCAL + p * PIECE

        @pl.when(c != p)
        def _():
            for s in range(SUB):
                passed(s).wait_recv()

        def tiles(t, _):
            for s, i in ((0, 4), (1, 8)):

                @pl.when((c == 1) & (p == 0) & (t == i))
                def _(s=s):
                    pass_on(s)

            @pl.when((p == 1) & (t == 1))
            def _():
                finish(0)

            late = jnp.maximum(t - 1, 0)
            project(base + t, t, block, lax.rem(t, 2), (late, block, lax.rem(late, 2)))

        lax.fori_loop(0, QT, tiles, None)
        turn(jnp.int32(QT - 1), block, (QT - 1) % 2)
        attend(block)

        @pl.when((c == 1) & (p == 0))
        def _():
            pass_on(2)

        def tiles_out(k, tiles):
            q, at = p * (PAIRS + 1) + k, lax.rem(k, 2)

            def put(j, value):
                acc[at, :, pl.ds(j * TILE, TILE)] = value

            output(base + QT, block, k, tiles, put)

            @pl.when(k >= 1)
            def _():
                add(p, k - 1, 2)

            @pl.when((q >= RING) & (lax.rem(q - RING, PAIRS + 1) < PAIRS))
            def _():
                exchange(q - RING, 2).wait_send()

            @pl.when((q >= RING) & (lax.rem(q - RING + PAIRS + 1, PAIRS + 1) == PAIRS))
            def _():
                exchange(q - RING, 1).wait_send()

            d_out[lax.rem(q, RING), :, pl.ds(0, tiles * TILE)] = acc[at, others, pl.ds(0, tiles * TILE)].astype(BF)

            @pl.when(k >= 1)
            def _():
                back(p, k - 1, 2).start()

            exchange(q, tiles).start()

        @pl.when(p == 1)
        def _():
            for s in range(SUB):
                swap(s).wait_send()
                link(s).wait_send()

        lax.fori_loop(0, PAIRS, lambda k, _: tiles_out(k, 2), None)
        tiles_out(jnp.int32(PAIRS), 1)

        @pl.when((c == 1) & (p == 0))
        def _():
            pass_on(SUB - 1)

    lax.fori_loop(0, 2, piece, None)
    for s in range(SUB):
        passed(s).wait_send()
    again = pltpu.make_async_copy(x, a.at[rows_of(me)], x_sem.at[0])
    again.start()

    def left(t, _):
        late = jnp.maximum(t - 1, 0)
        project(LATE + t, t, peer, lax.rem(t, 2), (late, peer, lax.rem(late, 2)))

    lax.fori_loop(0, LATER, left, None)
    turn(jnp.int32(LATER - 1), peer, (LATER - 1) % 2)
    finish(1)

    def own_chip(i, _):
        attend((1 - far) * 2 + i)

    lax.fori_loop(0, 2, own_chip, None)
    for q in range(2 * (PAIRS + 1) - RING, 2 * (PAIRS + 1)):
        exchange(jnp.int32(q), 1 if q % (PAIRS + 1) == PAIRS else 2).wait_send()

    def give(k, tiles):
        return remote(a.at[rows_of(across), some(k, tiles)], a.at[rows_of(across), some(k, tiles)], l_s.at[k], l_r.at[k], peer)

    def tiles_peer(k, tiles):
        def put(j, value):
            a[rows_of(across), pl.ds(pl.multiple_of(k * 2 * TILE + j * TILE, TILE), TILE)] = value.astype(BF)

        output(REMOTE, peer, k, tiles, put)

        @pl.when(k >= 1)
        def _():
            give(k - 1, 2).start()

    lax.fori_loop(0, PAIRS, lambda k, _: tiles_peer(k, 2), None)
    tiles_peer(jnp.int32(PAIRS), 1)

    again.wait()
    give(PAIRS, 1).start()

    def tiles_mine(k, tiles):
        def put(j, value):
            acc[0, :, pl.ds(j * TILE, TILE)] = value

        output(REMOTE + OU, me, k, tiles, put)
        here, width = some(k, tiles), pl.ds(0, tiles * TILE)
        give(k, tiles).wait_recv()
        for half in range(2):
            remote(y.at[sums(0), here], r_in.at[pl.ds(half * 128, 128), here], rs_s.at[0, k], rs_r.at[half, k], across).wait_recv()
        total = acc[0, :, width] + a[rows_of(diagonal), here].astype(F32) + r_in[:, here].astype(F32)
        for p in range(2):
            back(p, k, tiles).wait_send()
        y[:, here] = (a[rows_of(me), here].astype(F32) + total).astype(BF)

    lax.fori_loop(0, PAIRS, lambda k, _: tiles_mine(k, 2), None)
    tiles_mine(jnp.int32(PAIRS), 1)
    for k in range(PAIRS + 1):
        tiles = 2 if k < PAIRS else 1
        give(k, tiles).wait_send()


def solution(mesh):
    tables = rope_tables()

    def step(x, gain, wq, wk, wv, wo):
        anywhere, vmem, dma = pl.BlockSpec(memory_space=pl.ANY), pltpu.VMEM, pltpu.SemaphoreType.DMA
        return pl.pallas_call(
            kernel,
            out_shape=pltpu.VMEM((ROWS, D), BF),
            in_specs=[anywhere] * 8,
            out_specs=pl.BlockSpec(memory_space=pltpu.VMEM),
            scratch_shapes=[
                vmem((D,), BF),
                vmem((4 * ROWS, D), BF),
                vmem((3 * HEADS + 1, 4 * ROWS, HEAD), BF),
                vmem((4 * ROWS, WIDTH), BF),
                vmem((SLOTS, D, TILE), BF),
                vmem((ROWS, D), BF),
                vmem((RING, 128, 2 * TILE), BF),
                vmem((RING, 128, 2 * TILE), BF),
                vmem((2, ROWS, 2 * TILE), F32),
                vmem((2, ROWS, TILE), BF),
                vmem((5 * ROWS, HEAD), F32),
                vmem((5 * ROWS, HEAD), F32),
                vmem((16, ROWS), F32),
                vmem((HEADS, HEAD + 8, ROWS), F32),
                dma((SLOTS, 4)),
                dma((SUB,)),
                dma((3,)),
                dma((SUB,)),
                dma((SUB,)),
                dma((SUB,)),
                dma((SUB,)),
                dma((SUB,)),
                dma((SUB,)),
                dma((RING,)),
                dma((RING,)),
                dma((2, PAIRS + 1)),
                dma((2, PAIRS + 1)),
                dma((PAIRS + 1,)),
                dma((PAIRS + 1,)),
            ],
            compiler_params=pltpu.CompilerParams(collective_id=0, has_side_effects=True, vmem_limit_bytes=63_600_000),
            name="layer",
        )(x, gain, wq, wk, wv, wo, *(jnp.asarray(t) for t in tables))

    tokens, columns = P(("dp", "tp"), None), P(None, "tp")
    return jax.shard_map(
        step,
        mesh=mesh,
        in_specs=(tokens, P(None), columns, columns, columns, P("tp", None)),
        out_specs=tokens,
        check_vma=False,
    )
```

```python
import functools

import jax
import jax.numpy as jnp
import numpy as np
from jax import lax
from jax.experimental import pallas as pl
from jax.experimental.pallas import tpu as pltpu
from jax.sharding import PartitionSpec as P

HEAD = 128
THETA = 10000
NEG = -1e30
HIDDEN = 2 * NEG
LOG2E = 1.4426950408889634
MESH = pl.DeviceIdType.MESH
BF, F32 = jnp.bfloat16, jnp.float32

D = 6656
ROWS = 256
HEADS = 13
WIDTH = HEADS * HEAD
TILE = 512
QT = 10
OT = D // TILE
PAIRS = OT // 2
OU = 4
SLOTS = 3
LATER = 2
LOCAL = 2 * QT - LATER
PIECE = QT + OU
LATE = LOCAL + 2 * PIECE
REMOTE = LATE + LATER
UNITS = REMOTE + 2 * OU
RING = 3
SUB = 4
PART = ROWS // SUB
STEPS = PART // 16
GROUPS = ((0, 1, 2, 3), (4, 5, 6, 7), (8, 9, 10, 11, 12))


def rope_tables():
    half = HEAD // 2
    place = np.arange(4 * ROWS, dtype=np.float32)[:, None]
    angle = place * np.power(np.float32(THETA), -np.arange(half, dtype=np.float32) / np.float32(half))
    cos, sin = np.cos(angle), np.sin(angle)
    cos = np.concatenate([np.concatenate([cos, cos], 1), np.ones((ROWS, HEAD))], 0)
    sin = np.concatenate([np.concatenate([-sin, sin], 1), np.zeros((ROWS, HEAD))], 0)
    return cos.astype(np.float32), sin.astype(np.float32)


def cols(n):
    return pl.ds(pl.multiple_of(n * TILE, TILE), TILE)


def rows_of(block):
    return pl.ds(pl.multiple_of(block * ROWS, ROWS), ROWS)


def pair(n):
    return pl.ds(pl.multiple_of(n * 2 * TILE, 2 * TILE), 2 * TILE)


def quarter(j):
    return pl.ds(pl.multiple_of(j * WIDTH, WIDTH), WIDTH)


def own_tile(i):
    return jnp.where(i < QT, i, i - QT + LATER)


def kernel(x, gain_h, wq, wk, wv, wo, cos_h, sin_h, y,
           gain, a, qkv, seen, w, r_in, d_out, d_in, acc, raw, cos, sin, top_s, mix_s,
           w_sem, x_sem, t_sem, swap_s, swap_r, link_s, link_r, pass_s, pass_r, d_s, d_r, rs_s, rs_r, l_s, l_r):
    me = lax.axis_index("tp")
    c = lax.rem(me, 2)
    far = 1 - lax.div(me, 2)
    peer = me + 1 - 2 * c
    across = far * 2 + c
    diagonal = far * 2 + 1 - c

    def remote(src, dst, s, r, to):
        return pltpu.make_async_remote_copy(src_ref=src, dst_ref=dst, send_sem=s, recv_sem=r, device_id={"tp": to}, device_id_type=MESH)

    def issue(g):
        slot = lax.rem(g, SLOTS)
        in_piece = lax.rem(jnp.maximum(g - LOCAL, 0), PIECE)
        out = (g >= REMOTE) | ((g >= LOCAL) & (g < LATE) & (in_piece >= QT))
        t = jnp.where(g < LOCAL, own_tile(g), jnp.where(g < LATE, in_piece, g - LATE))
        u = jnp.where(g >= REMOTE, lax.rem(jnp.maximum(g - REMOTE, 0), OU), jnp.maximum(in_piece - QT, 0))
        project = jnp.logical_not(out)
        for i, ref in enumerate((wq, wk, wv)):

            @pl.when(project & (t >= 3 * i) & (t < 3 * i + 3))
            def _(i=i, ref=ref):
                for j in range(4):
                    pltpu.make_async_copy(ref.at[quarter(j), cols(lax.rem(t, 3))], w.at[slot, quarter(j)], w_sem.at[slot, j]).start()

        @pl.when(project & (t == QT - 1))
        def _():
            for j, ref in enumerate((wq, wk, wv, wv)):
                pltpu.make_async_copy(ref.at[:, pl.ds(3 * TILE, HEAD)], w.at[slot, :, pl.ds(j * HEAD, HEAD)], w_sem.at[slot, j]).start()

        for j in range(4):

            @pl.when(out & (g < UNITS) & (u * 4 + j < OT))
            def _(j=j):
                pltpu.make_async_copy(wo.at[:, cols(u * 4 + j)], w.at[slot, quarter(j)], w_sem.at[slot, j]).start()

    def fetched(slot, j):
        pltpu.make_async_copy(wo.at[:, pl.ds(0, TILE)], w.at[slot, quarter(j)], w_sem.at[slot, j]).wait()

    def part(block, s):
        return a.at[pl.ds(pl.multiple_of(block * ROWS + s * PART, PART), PART)]

    def swap(s):
        return remote(part(me, s), part(me, s), swap_s.at[s], swap_r.at[s], peer)

    def link(s):
        return remote(part(me, s), part(me, s), link_s.at[s], link_r.at[s], across)

    def passed(s):
        return remote(part(across, s), part(across, s), pass_s.at[s], pass_r.at[s], peer)

    def raw_link():
        return remote(x.at[pl.ds(0, PART)], part(me, 0), link_s.at[0], link_r.at[0], across)

    def pass_on(s):
        link(s).wait_recv()
        passed(s).start()

    loads = [pltpu.make_async_copy(x.at[pl.ds(s * PART, PART)], r_in.at[pl.ds(s * PART, PART)], x_sem.at[s]) for s in range(SUB)]
    tables = [pltpu.make_async_copy(cos_h, cos, t_sem.at[0]), pltpu.make_async_copy(sin_h, sin, t_sem.at[1])]
    gains = pltpu.make_async_copy(gain_h, gain, t_sem.at[2])
    barrier = pltpu.get_barrier_semaphore()
    for to in (peer, across, diagonal):
        pl.semaphore_signal(barrier, inc=1, device_id={"tp": to}, device_id_type=MESH)
    gains.start()
    for copy in loads:
        copy.start()
    for copy in tables:
        copy.start()

    pl.semaphore_wait(barrier, 3)

    @pl.when(c == 0)
    def _():
        raw_link().start()

    def norm(get, block, at):
        wide = get().astype(F32)
        scale = lax.rsqrt(jnp.mean(wide * wide, -1, keepdims=True) + 1e-6)
        a[pl.ds(pl.multiple_of(block * ROWS + at, 16), 16), :] = (wide * scale * gain[...].reshape(1, D).astype(F32)).astype(BF)

    def send(s):
        swap(s).start()

        @pl.when((c == 0) & (s > 0))
        def _():
            link(s).start()

    def own(i, _):
        s = lax.div(i, STEPS)

        @pl.when(lax.rem(i, STEPS) == 0)
        def _():
            pltpu.make_async_copy(x.at[pl.ds(0, PART)], r_in.at[pl.ds(0, PART)], x_sem.at[s]).wait()

        norm(lambda: r_in[pl.ds(pl.multiple_of(i * 16, 16), 16), :], me, i * 16)

        for g, at in ((0, 1), (1, (SUB - 1) * STEPS + 1)):

            @pl.when(i == at)
            def _(g=g):
                issue(jnp.int32(g))

    gains.wait()

    def own_and_send(i, _):
        own(i, _)

        @pl.when((lax.rem(i, STEPS) == 0) & (i > 0))
        def _():
            send(lax.div(i, STEPS) - 1)

    lax.fori_loop(0, SUB * STEPS, own_and_send, None)
    send(SUB - 1)
    for copy in tables:
        copy.wait()

    def turn(t, block, at):
        for i in range(4):
            slot = jnp.where(t < QT - 1, lax.div(t, 3) * HEADS + lax.rem(t, 3) * 4 + i, min(i * HEADS + HEADS - 1, 3 * HEADS))
            plain = ((t >= 6) & (t < QT - 1)) | ((t == QT - 1) & (i >= 2))
            angles = pl.ds(pl.multiple_of(jnp.where(plain, 4, block) * ROWS, ROWS), ROWS)
            v = raw[at, :, pl.ds(i * HEAD, HEAD)].astype(F32)
            v = v * cos[angles, :] + pltpu.roll(v, HEAD // 2, 1) * sin[angles, :]
            qkv[slot, rows_of(block), :] = v.astype(BF)

    def project(g, t, block, here, before):
        issue(g + SLOTS - 1)
        slot = lax.rem(g, SLOTS)
        for j in range(4):
            fetched(slot, j)
        raw[here] = jnp.dot(a[rows_of(block), :], w[slot], preferred_element_type=F32).astype(BF)
        turn(*before)

    def local(i, _):
        block = jnp.where(i < QT, me, peer)
        late = jnp.maximum(i - 1, 0)

        @pl.when(i == QT)
        def _():
            for s in range(SUB):
                swap(s).wait_recv()

        @pl.when((c == 1) & (i == 14))
        def _():
            for s in range(SUB):
                link(s).start()

        @pl.when((c == 0) & (i == 6))
        def _():
            link(0).wait_recv()

            def step(n, _):
                norm(lambda: a[pl.ds(pl.multiple_of(across * ROWS + n * 16, 16), 16), :], across, n * 16)

            lax.fori_loop(0, STEPS, step, None)

        @pl.when((c == 0) & (i == 7))
        def _():
            passed(0).start()

        for s, at in ((1, 10), (2, 14), (3, 17)):

            @pl.when((c == 0) & (i == at))
            def _(s=s):
                pass_on(s)

        project(i, own_tile(i), block, lax.rem(i, 2), (own_tile(late), jnp.where(late < QT, me, peer), lax.rem(late, 2)))

    raw[...] = jnp.zeros_like(raw)
    lax.fori_loop(0, LOCAL, local, None)
    turn(jnp.int32(QT - 1), peer, (LOCAL - 1) % 2)


    def attend(block):
        e = HEAD**-0.5 * LOG2E
        top_s[...] = jnp.full(top_s.shape, NEG, F32)
        mix_s[...] = jnp.zeros(mix_s.shape, F32)
        ones = jnp.ones((8, ROWS), BF)

        def keys(j, masked):

            def score(heads):
                return [
                    lax.dot_general(qkv[HEADS + h, rows_of(j), :], qkv[h, rows_of(block), :], (((1,), (1,)), ((), ())), preferred_element_type=F32)
                    for h in heads
                ]

            ahead = score(GROUPS[0])
            for at, heads in enumerate(GROUPS):
                scores = ahead
                if at + 1 < len(GROUPS):
                    ahead = score(GROUPS[at + 1])
                weights, keeps = [], []
                for h, s in zip(heads, scores):
                    if masked:
                        s = jnp.where(lax.broadcasted_iota(jnp.int32, s.shape, 1) >= lax.broadcasted_iota(jnp.int32, s.shape, 0), s, HIDDEN)
                    old = top_s[h : h + 1, :]
                    top = jnp.maximum(old, s.max(axis=0, keepdims=True))
                    top_s[h : h + 1, :] = top
                    weights.append(jnp.exp2((s - top) * e).astype(BF))
                    keeps.append(jnp.exp2((old - top) * e))
                for h, p, keep in zip(heads, weights, keeps):
                    values = jnp.concatenate([qkv[2 * HEADS + h, rows_of(j), :].T, ones], axis=0)
                    mix_s[h] = mix_s[h] * keep + jnp.dot(values, p, preferred_element_type=F32)

        lax.fori_loop(0, block, lambda j, _: keys(j, False), None)
        keys(block, True)
        for h in range(HEADS):
            done = mix_s[h, :HEAD, :] * (1 / mix_s[h, HEAD : HEAD + 1, :])
            seen[rows_of(block), pl.ds(h * HEAD, HEAD)] = done.T.astype(BF)

    def output(base, block, k, tiles, put):
        slot = lax.rem(base + lax.div(k, 2), SLOTS)
        first = lax.rem(k, 2) * 2

        @pl.when(first == 0)
        def _():
            issue(base + lax.div(k, 2) + SLOTS - 1)

        for j in range(tiles):
            fetched(slot, first + j)
        for j in range(tiles):
            put(j, jnp.dot(seen[rows_of(block), :], w[slot, quarter(first + j), :], preferred_element_type=F32))

    def some(k, tiles):
        return pair(k) if tiles == 2 else pl.ds(PAIRS * 2 * TILE, TILE)

    mine = pl.ds(pl.multiple_of(c * 128, 128), 128)
    others = pl.ds(pl.multiple_of((1 - c) * 128, 128), 128)

    def exchange(q, tiles):
        slot, width = lax.rem(q, RING), pl.ds(0, tiles * TILE)
        return remote(d_out.at[slot, :, width], d_in.at[slot, :, width], d_s.at[slot], d_r.at[slot], peer)

    def sums(p):
        return pl.ds(pl.multiple_of(p * 128, 128), 128)

    def back(p, k, tiles):
        return remote(y.at[sums(p), some(k, tiles)], r_in.at[mine, some(k, tiles)], rs_s.at[p, k], rs_r.at[c, k], far * 2 + p)

    def add(p, k, tiles):
        q, width = p * (PAIRS + 1) + k, pl.ds(0, tiles * TILE)
        exchange(q, tiles).wait_recv()
        total = acc[lax.rem(k, 2), mine, width] + d_in[lax.rem(q, RING), :, width].astype(F32)
        y[sums(p), some(k, tiles)] = total.astype(BF)

    def finish(p):
        add(p, jnp.int32(PAIRS), 1)
        back(p, PAIRS, 1).start()

    def piece(p, _):
        block = far * 2 + p
        base = LOCAL + p * PIECE

        @pl.when(c != p)
        def _():
            for s in range(SUB):
                passed(s).wait_recv()

        def tiles(t, _):
            for s, i in ((0, 4), (1, 8)):

                @pl.when((c == 1) & (p == 0) & (t == i))
                def _(s=s):
                    pass_on(s)

            @pl.when((p == 1) & (t == 1))
            def _():
                finish(0)

            late = jnp.maximum(t - 1, 0)
            project(base + t, t, block, lax.rem(t, 2), (late, block, lax.rem(late, 2)))

        lax.fori_loop(0, QT, tiles, None)
        turn(jnp.int32(QT - 1), block, (QT - 1) % 2)
        attend(block)

        @pl.when((c == 1) & (p == 0))
        def _():
            pass_on(2)

        def tiles_out(k, tiles):
            q, at = p * (PAIRS + 1) + k, lax.rem(k, 2)

            def put(j, value):
                acc[at, :, pl.ds(j * TILE, TILE)] = value

            output(base + QT, block, k, tiles, put)

            @pl.when(k >= 1)
            def _():
                add(p, k - 1, 2)

            @pl.when((q >= RING) & (lax.rem(q - RING, PAIRS + 1) < PAIRS))
            def _():
                exchange(q - RING, 2).wait_send()

            @pl.when((q >= RING) & (lax.rem(q - RING + PAIRS + 1, PAIRS + 1) == PAIRS))
            def _():
                exchange(q - RING, 1).wait_send()

            d_out[lax.rem(q, RING), :, pl.ds(0, tiles * TILE)] = acc[at, others, pl.ds(0, tiles * TILE)].astype(BF)

            @pl.when(k >= 1)
            def _():
                back(p, k - 1, 2).start()

            exchange(q, tiles).start()

        @pl.when(p == 1)
        def _():
            for s in range(SUB):
                swap(s).wait_send()
                link(s).wait_send()

        def pairs_out(k, _):
            @pl.when((c == 1) & (p == 0) & (k == 5))
            def _():
                pass_on(SUB - 1)

            tiles_out(k, 2)

        lax.fori_loop(0, PAIRS, pairs_out, None)
        tiles_out(jnp.int32(PAIRS), 1)

    lax.fori_loop(0, 2, piece, None)
    for s in range(SUB):
        passed(s).wait_send()
    again = pltpu.make_async_copy(x, a.at[rows_of(me)], x_sem.at[0])
    again.start()

    def left(t, _):
        late = jnp.maximum(t - 1, 0)
        project(LATE + t, t, peer, lax.rem(t, 2), (late, peer, lax.rem(late, 2)))

    lax.fori_loop(0, LATER, left, None)
    turn(jnp.int32(LATER - 1), peer, (LATER - 1) % 2)
    finish(1)

    def own_chip(i, _):
        attend((1 - far) * 2 + i)

    lax.fori_loop(0, 2, own_chip, None)
    for q in range(2 * (PAIRS + 1) - RING, 2 * (PAIRS + 1)):
        exchange(jnp.int32(q), 1 if q % (PAIRS + 1) == PAIRS else 2).wait_send()

    def give(k, tiles):
        return remote(a.at[rows_of(across), some(k, tiles)], a.at[rows_of(across), some(k, tiles)], l_s.at[k], l_r.at[k], peer)

    def tiles_peer(k, tiles):
        def put(j, value):
            a[rows_of(across), pl.ds(pl.multiple_of(k * 2 * TILE + j * TILE, TILE), TILE)] = value.astype(BF)

        output(REMOTE, peer, k, tiles, put)

        @pl.when(k >= 1)
        def _():
            give(k - 1, 2).start()

    lax.fori_loop(0, PAIRS, lambda k, _: tiles_peer(k, 2), None)
    tiles_peer(jnp.int32(PAIRS), 1)

    again.wait()
    give(PAIRS, 1).start()

    def tiles_mine(k, tiles):
        def put(j, value):
            acc[0, :, pl.ds(j * TILE, TILE)] = value

        output(REMOTE + OU, me, k, tiles, put)
        here, width = some(k, tiles), pl.ds(0, tiles * TILE)
        give(k, tiles).wait_recv()
        for half in range(2):
            remote(y.at[sums(0), here], r_in.at[pl.ds(half * 128, 128), here], rs_s.at[0, k], rs_r.at[half, k], across).wait_recv()
        total = acc[0, :, width] + a[rows_of(diagonal), here].astype(F32) + r_in[:, here].astype(F32)
        for p in range(2):
            back(p, k, tiles).wait_send()
        y[:, here] = (a[rows_of(me), here].astype(F32) + total).astype(BF)

    lax.fori_loop(0, PAIRS, lambda k, _: tiles_mine(k, 2), None)
    tiles_mine(jnp.int32(PAIRS), 1)
    for k in range(PAIRS + 1):
        tiles = 2 if k < PAIRS else 1
        give(k, tiles).wait_send()


def solution(mesh):
    tables = rope_tables()

    def step(x, gain, wq, wk, wv, wo):
        anywhere, vmem, dma = pl.BlockSpec(memory_space=pl.ANY), pltpu.VMEM, pltpu.SemaphoreType.DMA
        return pl.pallas_call(
            kernel,
            out_shape=pltpu.VMEM((ROWS, D), BF),
            in_specs=[anywhere] * 8,
            out_specs=pl.BlockSpec(memory_space=pltpu.VMEM),
            scratch_shapes=[
                vmem((D,), BF),
                vmem((4 * ROWS, D), BF),
                vmem((3 * HEADS + 1, 4 * ROWS, HEAD), BF),
                vmem((4 * ROWS, WIDTH), BF),
                vmem((SLOTS, D, TILE), BF),
                vmem((ROWS, D), BF),
                vmem((RING, 128, 2 * TILE), BF),
                vmem((RING, 128, 2 * TILE), BF),
                vmem((2, ROWS, 2 * TILE), F32),
                vmem((2, ROWS, TILE), BF),
                vmem((5 * ROWS, HEAD), F32),
                vmem((5 * ROWS, HEAD), F32),
                vmem((16, ROWS), F32),
                vmem((HEADS, HEAD + 8, ROWS), F32),
                dma((SLOTS, 4)),
                dma((SUB,)),
                dma((3,)),
                dma((SUB,)),
                dma((SUB,)),
                dma((SUB,)),
                dma((SUB,)),
                dma((SUB,)),
                dma((SUB,)),
                dma((RING,)),
                dma((RING,)),
                dma((2, PAIRS + 1)),
                dma((2, PAIRS + 1)),
                dma((PAIRS + 1,)),
                dma((PAIRS + 1,)),
            ],
            compiler_params=pltpu.CompilerParams(collective_id=0, has_side_effects=True, vmem_limit_bytes=63_600_000),
            name="layer",
        )(x, gain, wq, wk, wv, wo, *(jnp.asarray(t) for t in tables))

    tokens, columns = P(("dp", "tp"), None), P(None, "tp")
    return jax.shard_map(
        step,
        mesh=mesh,
        in_specs=(tokens, P(None), columns, columns, columns, P("tp", None)),
        out_specs=tokens,
        check_vma=False,
    )
```

```python
import functools

import jax
import jax.numpy as jnp
import numpy as np
from jax import lax
from jax.experimental import pallas as pl
from jax.experimental.pallas import tpu as pltpu
from jax.sharding import PartitionSpec as P

HEAD = 128
THETA = 10000
NEG = -1e30
HIDDEN = 2 * NEG
LOG2E = 1.4426950408889634
MESH = pl.DeviceIdType.MESH
BF, F32 = jnp.bfloat16, jnp.float32

D = 6656
ROWS = 256
HEADS = 13
WIDTH = HEADS * HEAD
TILE = 512
QT = 10
OT = D // TILE
PAIRS = OT // 2
OU = 4
SLOTS = 3
LATER = 2
LOCAL = 2 * QT - LATER
PIECE = QT + OU
LATE = LOCAL + 2 * PIECE
REMOTE = LATE + LATER
UNITS = REMOTE + 2 * OU
RING = 3
SUB = 4
PART = ROWS // SUB
STEPS = PART // 16
GROUPS = ((0, 1, 2, 3), (4, 5, 6, 7), (8, 9, 10, 11, 12))


def rope_tables():
    half = HEAD // 2
    place = np.arange(4 * ROWS, dtype=np.float32)[:, None]
    angle = place * np.power(np.float32(THETA), -np.arange(half, dtype=np.float32) / np.float32(half))
    cos, sin = np.cos(angle), np.sin(angle)
    cos = np.concatenate([np.concatenate([cos, cos], 1), np.ones((ROWS, HEAD))], 0)
    sin = np.concatenate([np.concatenate([-sin, sin], 1), np.zeros((ROWS, HEAD))], 0)
    return cos.astype(np.float32), sin.astype(np.float32)


def cols(n):
    return pl.ds(pl.multiple_of(n * TILE, TILE), TILE)


def rows_of(block):
    return pl.ds(pl.multiple_of(block * ROWS, ROWS), ROWS)


def pair(n):
    return pl.ds(pl.multiple_of(n * 2 * TILE, 2 * TILE), 2 * TILE)


def quarter(j):
    return pl.ds(pl.multiple_of(j * WIDTH, WIDTH), WIDTH)


def own_tile(i):
    return jnp.where(i < QT, i, i - QT + LATER)


def kernel(x, gain_h, wq, wk, wv, wo, cos_h, sin_h, y,
           gain, a, qkv, seen, w, r_in, d_out, d_in, acc, raw, cos, sin, top_s, mix_s,
           w_sem, x_sem, t_sem, swap_s, swap_r, link_s, link_r, pass_s, pass_r, d_s, d_r, rs_s, rs_r, l_s, l_r):
    me = lax.axis_index("tp")
    c = lax.rem(me, 2)
    far = 1 - lax.div(me, 2)
    peer = me + 1 - 2 * c
    across = far * 2 + c
    diagonal = far * 2 + 1 - c

    def remote(src, dst, s, r, to):
        return pltpu.make_async_remote_copy(src_ref=src, dst_ref=dst, send_sem=s, recv_sem=r, device_id={"tp": to}, device_id_type=MESH)

    def issue(g):
        slot = lax.rem(g, SLOTS)
        in_piece = lax.rem(jnp.maximum(g - LOCAL, 0), PIECE)
        out = (g >= REMOTE) | ((g >= LOCAL) & (g < LATE) & (in_piece >= QT))
        t = jnp.where(g < LOCAL, own_tile(g), jnp.where(g < LATE, in_piece, g - LATE))
        u = jnp.where(g >= REMOTE, lax.rem(jnp.maximum(g - REMOTE, 0), OU), jnp.maximum(in_piece - QT, 0))
        project = jnp.logical_not(out)
        for i, ref in enumerate((wq, wk, wv)):

            @pl.when(project & (t >= 3 * i) & (t < 3 * i + 3))
            def _(i=i, ref=ref):
                for j in range(4):
                    pltpu.make_async_copy(ref.at[quarter(j), cols(lax.rem(t, 3))], w.at[slot, quarter(j)], w_sem.at[slot, j]).start()

        @pl.when(project & (t == QT - 1))
        def _():
            for j, ref in enumerate((wq, wk, wv, wv)):
                pltpu.make_async_copy(ref.at[:, pl.ds(3 * TILE, HEAD)], w.at[slot, :, pl.ds(j * HEAD, HEAD)], w_sem.at[slot, j]).start()

        for j in range(4):

            @pl.when(out & (g < UNITS) & (u * 4 + j < OT))
            def _(j=j):
                pltpu.make_async_copy(wo.at[:, cols(u * 4 + j)], w.at[slot, quarter(j)], w_sem.at[slot, j]).start()

    def fetched(slot, j):
        pltpu.make_async_copy(wo.at[:, pl.ds(0, TILE)], w.at[slot, quarter(j)], w_sem.at[slot, j]).wait()

    def part(block, s):
        return a.at[pl.ds(pl.multiple_of(block * ROWS + s * PART, PART), PART)]

    def swap(s):
        return remote(part(me, s), part(me, s), swap_s.at[s], swap_r.at[s], peer)

    def link(s):
        return remote(part(me, s), part(me, s), link_s.at[s], link_r.at[s], across)

    def passed(s):
        return remote(part(across, s), part(across, s), pass_s.at[s], pass_r.at[s], peer)

    def raw_link():
        return remote(x.at[pl.ds(0, PART)], part(me, 0), link_s.at[0], link_r.at[0], across)

    def pass_on(s):
        link(s).wait_recv()
        passed(s).start()

    loads = [pltpu.make_async_copy(x.at[pl.ds(s * PART, PART)], r_in.at[pl.ds(s * PART, PART)], x_sem.at[s]) for s in range(SUB)]
    tables = [pltpu.make_async_copy(cos_h, cos, t_sem.at[0]), pltpu.make_async_copy(sin_h, sin, t_sem.at[1])]
    gains = pltpu.make_async_copy(gain_h, gain, t_sem.at[2])
    barrier = pltpu.get_barrier_semaphore()
    for to in (peer, across, diagonal):
        pl.semaphore_signal(barrier, inc=1, device_id={"tp": to}, device_id_type=MESH)
    gains.start()
    for copy in loads:
        copy.start()
    for copy in tables:
        copy.start()

    pl.semaphore_wait(barrier, 3)

    @pl.when(c == 0)
    def _():
        raw_link().start()

    def norm(get, block, at):
        wide = get().astype(F32)
        scale = lax.rsqrt(jnp.mean(wide * wide, -1, keepdims=True) + 1e-6)
        a[pl.ds(pl.multiple_of(block * ROWS + at, 16), 16), :] = (wide * scale * gain[...].reshape(1, D).astype(F32)).astype(BF)

    def send(s):
        swap(s).start()

        @pl.when((c == 0) & (s > 0))
        def _():
            link(s).start()

    def own(i, _):
        s = lax.div(i, STEPS)

        @pl.when(lax.rem(i, STEPS) == 0)
        def _():
            pltpu.make_async_copy(x.at[pl.ds(0, PART)], r_in.at[pl.ds(0, PART)], x_sem.at[s]).wait()

        norm(lambda: r_in[pl.ds(pl.multiple_of(i * 16, 16), 16), :], me, i * 16)

        for g, at in ((0, 1), (1, (SUB - 1) * STEPS + 1)):

            @pl.when(i == at)
            def _(g=g):
                issue(jnp.int32(g))

    gains.wait()

    def own_and_send(i, _):
        own(i, _)

        @pl.when((lax.rem(i, STEPS) == 0) & (i > 0))
        def _():
            send(lax.div(i, STEPS) - 1)

    lax.fori_loop(0, SUB * STEPS, own_and_send, None)
    send(SUB - 1)
    for copy in tables:
        copy.wait()

    def turn(t, block, at):
        for i in range(4):
            slot = jnp.where(t < QT - 1, lax.div(t, 3) * HEADS + lax.rem(t, 3) * 4 + i, min(i * HEADS + HEADS - 1, 3 * HEADS))
            plain = ((t >= 6) & (t < QT - 1)) | ((t == QT - 1) & (i >= 2))
            angles = pl.ds(pl.multiple_of(jnp.where(plain, 4, block) * ROWS, ROWS), ROWS)
            v = raw[at, :, pl.ds(i * HEAD, HEAD)].astype(F32)
            v = v * cos[angles, :] + pltpu.roll(v, HEAD // 2, 1) * sin[angles, :]
            qkv[slot, rows_of(block), :] = v.astype(BF)

    def project(g, t, block, here, before):
        issue(g + SLOTS - 1)
        slot = lax.rem(g, SLOTS)
        for j in range(4):
            fetched(slot, j)
        raw[here] = jnp.dot(a[rows_of(block), :], w[slot], preferred_element_type=F32).astype(BF)
        turn(*before)

    def local(i, _):
        block = jnp.where(i < QT, me, peer)
        late = jnp.maximum(i - 1, 0)

        @pl.when(i == QT)
        def _():
            for s in range(SUB):
                swap(s).wait_recv()

        @pl.when((c == 1) & (i == 15 - far))
        def _():
            for s in range(SUB):
                link(s).start()

        @pl.when((c == 0) & (i == 6))
        def _():
            link(0).wait_recv()

            def step(n, _):
                norm(lambda: a[pl.ds(pl.multiple_of(across * ROWS + n * 16, 16), 16), :], across, n * 16)

            lax.fori_loop(0, STEPS, step, None)

        @pl.when((c == 0) & (i == 7))
        def _():
            passed(0).start()

        for s, at in ((1, 10), (2, 14), (3, 17)):

            @pl.when((c == 0) & (i == at))
            def _(s=s):
                pass_on(s)

        project(i, own_tile(i), block, lax.rem(i, 2), (own_tile(late), jnp.where(late < QT, me, peer), lax.rem(late, 2)))

    raw[...] = jnp.zeros_like(raw)
    lax.fori_loop(0, LOCAL, local, None)
    turn(jnp.int32(QT - 1), peer, (LOCAL - 1) % 2)


    def attend(block):
        e = HEAD**-0.5 * LOG2E
        top_s[...] = jnp.full(top_s.shape, NEG, F32)
        mix_s[...] = jnp.zeros(mix_s.shape, F32)
        ones = jnp.ones((8, ROWS), BF)

        def keys(j, masked):

            def score(heads):
                return [
                    lax.dot_general(qkv[HEADS + h, rows_of(j), :], qkv[h, rows_of(block), :], (((1,), (1,)), ((), ())), preferred_element_type=F32)
                    for h in heads
                ]

            ahead = score(GROUPS[0])
            for at, heads in enumerate(GROUPS):
                scores = ahead
                if at + 1 < len(GROUPS):
                    ahead = score(GROUPS[at + 1])
                weights, keeps = [], []
                for h, s in zip(heads, scores):
                    if masked:
                        s = jnp.where(lax.broadcasted_iota(jnp.int32, s.shape, 1) >= lax.broadcasted_iota(jnp.int32, s.shape, 0), s, HIDDEN)
                    old = top_s[h : h + 1, :]
                    top = jnp.maximum(old, s.max(axis=0, keepdims=True))
                    top_s[h : h + 1, :] = top
                    weights.append(jnp.exp2((s - top) * e).astype(BF))
                    keeps.append(jnp.exp2((old - top) * e))
                for h, p, keep in zip(heads, weights, keeps):
                    values = jnp.concatenate([qkv[2 * HEADS + h, rows_of(j), :].T, ones], axis=0)
                    mix_s[h] = mix_s[h] * keep + jnp.dot(values, p, preferred_element_type=F32)

        lax.fori_loop(0, block, lambda j, _: keys(j, False), None)
        keys(block, True)
        for h in range(HEADS):
            done = mix_s[h, :HEAD, :] * (1 / mix_s[h, HEAD : HEAD + 1, :])
            seen[rows_of(block), pl.ds(h * HEAD, HEAD)] = done.T.astype(BF)

    def output(base, block, k, tiles, put):
        slot = lax.rem(base + lax.div(k, 2), SLOTS)
        first = lax.rem(k, 2) * 2

        @pl.when(first == 0)
        def _():
            issue(base + lax.div(k, 2) + SLOTS - 1)

        for j in range(tiles):
            fetched(slot, first + j)
        for j in range(tiles):
            put(j, jnp.dot(seen[rows_of(block), :], w[slot, quarter(first + j), :], preferred_element_type=F32))

    def some(k, tiles):
        return pair(k) if tiles == 2 else pl.ds(PAIRS * 2 * TILE, TILE)

    mine = pl.ds(pl.multiple_of(c * 128, 128), 128)
    others = pl.ds(pl.multiple_of((1 - c) * 128, 128), 128)

    def exchange(q, tiles):
        slot, width = lax.rem(q, RING), pl.ds(0, tiles * TILE)
        return remote(d_out.at[slot, :, width], d_in.at[slot, :, width], d_s.at[slot], d_r.at[slot], peer)

    def sums(p):
        return pl.ds(pl.multiple_of(p * 128, 128), 128)

    def back(p, k, tiles):
        return remote(y.at[sums(p), some(k, tiles)], r_in.at[mine, some(k, tiles)], rs_s.at[p, k], rs_r.at[c, k], far * 2 + p)

    def add(p, k, tiles):
        q, width = p * (PAIRS + 1) + k, pl.ds(0, tiles * TILE)
        exchange(q, tiles).wait_recv()
        total = acc[lax.rem(k, 2), mine, width] + d_in[lax.rem(q, RING), :, width].astype(F32)
        y[sums(p), some(k, tiles)] = total.astype(BF)

    def finish(p):
        add(p, jnp.int32(PAIRS), 1)
        back(p, PAIRS, 1).start()

    def piece(p, _):
        block = far * 2 + p
        base = LOCAL + p * PIECE

        @pl.when(c != p)
        def _():
            for s in range(SUB):
                passed(s).wait_recv()

        def tiles(t, _):
            for s, i in ((0, 4), (1, 8)):

                @pl.when((c == 1) & (p == 0) & (t == i))
                def _(s=s):
                    pass_on(s)

            @pl.when((p == 1) & (t == 1))
            def _():
                finish(0)

            late = jnp.maximum(t - 1, 0)
            project(base + t, t, block, lax.rem(t, 2), (late, block, lax.rem(late, 2)))

        lax.fori_loop(0, QT, tiles, None)
        turn(jnp.int32(QT - 1), block, (QT - 1) % 2)
        attend(block)

        @pl.when((c == 1) & (p == 0))
        def _():
            pass_on(2)

        def tiles_out(k, tiles):
            q, at = p * (PAIRS + 1) + k, lax.rem(k, 2)

            def put(j, value):
                acc[at, :, pl.ds(j * TILE, TILE)] = value

            output(base + QT, block, k, tiles, put)

            @pl.when(k >= 1)
            def _():
                add(p, k - 1, 2)

            @pl.when((q >= RING) & (lax.rem(q - RING, PAIRS + 1) < PAIRS))
            def _():
                exchange(q - RING, 2).wait_send()

            @pl.when((q >= RING) & (lax.rem(q - RING + PAIRS + 1, PAIRS + 1) == PAIRS))
            def _():
                exchange(q - RING, 1).wait_send()

            d_out[lax.rem(q, RING), :, pl.ds(0, tiles * TILE)] = acc[at, others, pl.ds(0, tiles * TILE)].astype(BF)

            @pl.when(k >= 1)
            def _():
                back(p, k - 1, 2).start()

            exchange(q, tiles).start()

        @pl.when(p == 1)
        def _():
            for s in range(SUB):
                swap(s).wait_send()
                link(s).wait_send()

        def pairs_out(k, _):
            @pl.when((c == 1) & (p == 0) & (k == 5))
            def _():
                pass_on(SUB - 1)

            tiles_out(k, 2)

        lax.fori_loop(0, PAIRS, pairs_out, None)
        tiles_out(jnp.int32(PAIRS), 1)

    lax.fori_loop(0, 2, piece, None)
    for s in range(SUB):
        passed(s).wait_send()
    again = pltpu.make_async_copy(x, a.at[rows_of(me)], x_sem.at[0])
    again.start()

    def left(t, _):
        late = jnp.maximum(t - 1, 0)
        project(LATE + t, t, peer, lax.rem(t, 2), (late, peer, lax.rem(late, 2)))

    lax.fori_loop(0, LATER, left, None)
    turn(jnp.int32(LATER - 1), peer, (LATER - 1) % 2)
    finish(1)

    def own_chip(i, _):
        attend((1 - far) * 2 + i)

    lax.fori_loop(0, 2, own_chip, None)
    for q in range(2 * (PAIRS + 1) - RING, 2 * (PAIRS + 1)):
        exchange(jnp.int32(q), 1 if q % (PAIRS + 1) == PAIRS else 2).wait_send()

    def give(k, tiles):
        return remote(a.at[rows_of(across), some(k, tiles)], a.at[rows_of(across), some(k, tiles)], l_s.at[k], l_r.at[k], peer)

    def tiles_peer(k, tiles):
        def put(j, value):
            a[rows_of(across), pl.ds(pl.multiple_of(k * 2 * TILE + j * TILE, TILE), TILE)] = value.astype(BF)

        output(REMOTE, peer, k, tiles, put)

        @pl.when(k >= 1)
        def _():
            give(k - 1, 2).start()

    lax.fori_loop(0, PAIRS, lambda k, _: tiles_peer(k, 2), None)
    tiles_peer(jnp.int32(PAIRS), 1)

    again.wait()
    give(PAIRS, 1).start()

    def tiles_mine(k, tiles):
        def put(j, value):
            acc[0, :, pl.ds(j * TILE, TILE)] = value

        output(REMOTE + OU, me, k, tiles, put)
        here, width = some(k, tiles), pl.ds(0, tiles * TILE)
        give(k, tiles).wait_recv()
        for half in range(2):
            remote(y.at[sums(0), here], r_in.at[pl.ds(half * 128, 128), here], rs_s.at[0, k], rs_r.at[half, k], across).wait_recv()
        total = acc[0, :, width] + a[rows_of(diagonal), here].astype(F32) + r_in[:, here].astype(F32)
        for p in range(2):
            back(p, k, tiles).wait_send()
        y[:, here] = (a[rows_of(me), here].astype(F32) + total).astype(BF)

    lax.fori_loop(0, PAIRS, lambda k, _: tiles_mine(k, 2), None)
    tiles_mine(jnp.int32(PAIRS), 1)
    for k in range(PAIRS + 1):
        tiles = 2 if k < PAIRS else 1
        give(k, tiles).wait_send()


def solution(mesh):
    tables = rope_tables()

    def step(x, gain, wq, wk, wv, wo):
        anywhere, vmem, dma = pl.BlockSpec(memory_space=pl.ANY), pltpu.VMEM, pltpu.SemaphoreType.DMA
        return pl.pallas_call(
            kernel,
            out_shape=pltpu.VMEM((ROWS, D), BF),
            in_specs=[anywhere] * 8,
            out_specs=pl.BlockSpec(memory_space=pltpu.VMEM),
            scratch_shapes=[
                vmem((D,), BF),
                vmem((4 * ROWS, D), BF),
                vmem((3 * HEADS + 1, 4 * ROWS, HEAD), BF),
                vmem((4 * ROWS, WIDTH), BF),
                vmem((SLOTS, D, TILE), BF),
                vmem((ROWS, D), BF),
                vmem((RING, 128, 2 * TILE), BF),
                vmem((RING, 128, 2 * TILE), BF),
                vmem((2, ROWS, 2 * TILE), F32),
                vmem((2, ROWS, TILE), BF),
                vmem((5 * ROWS, HEAD), F32),
                vmem((5 * ROWS, HEAD), F32),
                vmem((16, ROWS), F32),
                vmem((HEADS, HEAD + 8, ROWS), F32),
                dma((SLOTS, 4)),
                dma((SUB,)),
                dma((3,)),
                dma((SUB,)),
                dma((SUB,)),
                dma((SUB,)),
                dma((SUB,)),
                dma((SUB,)),
                dma((SUB,)),
                dma((RING,)),
                dma((RING,)),
                dma((2, PAIRS + 1)),
                dma((2, PAIRS + 1)),
                dma((PAIRS + 1,)),
                dma((PAIRS + 1,)),
            ],
            compiler_params=pltpu.CompilerParams(collective_id=0, has_side_effects=True, vmem_limit_bytes=63_600_000),
            name="layer",
        )(x, gain, wq, wk, wv, wo, *(jnp.asarray(t) for t in tables))

    tokens, columns = P(("dp", "tp"), None), P(None, "tp")
    return jax.shard_map(
        step,
        mesh=mesh,
        in_specs=(tokens, P(None), columns, columns, columns, P("tp", None)),
        out_specs=tokens,
        check_vma=False,
    )
```
